256 devices in a mesh: row: 16 (over y, x), col: 16 (over z, core).
Axes of the slice: x: 4, y: 4, z: 8, core: 2. Of those that a mesh axis runs over, the one named last changes fastest.
Arguments:
- matrix: float32 [2, 16, 256, 2, 16, 256], P(None, 'row', None, None, 'col'), as said below
Outputs:
- factored: float32 [2, 16, 256, 2, 16, 256], P(None, 'row', None, None, 'col')
Inputs may be any that keep to these rules, and one draw needn't show every extreme that they name: `matrix`: symmetric and positive definite.
All inputs are finite; a program needn't handle non-finite values.
Results may differ from the reference program's by a relative error of at most 0.0001.
Values sent between devices are 32-bit elements; how exact they have to be, the bound alone decides.
A program may use at most 128 MiB of HBM per device.

```python
import jax
import jax.numpy as jnp
from jax import lax

B = 256
MR = 2
STEPS = 8
MC = 2
N_ROW = 16
N_COL = 16


def draw_matrix(key, part):
    order = MR * N_ROW * B
    inner_count = order // 4
    first, second = jax.random.split(key, 2)
    factor_g = jax.random.normal(first, (order, inner_count), jnp.float32)
    product = jnp.dot(factor_g, factor_g.T, precision=lax.Precision.HIGHEST, preferred_element_type=jnp.float32)
    product = product * (1.0 / inner_count)
    product = 0.5 * (product + product.T)
    diag_vals = jax.random.uniform(second, (order,), jnp.float32, 0.5, 1.5)
    result = product + jnp.diag(diag_vals)
    return result.reshape(MR, N_ROW, B, MC, N_COL, B)


def setup_inputs(seed: int = 0) -> dict:
    streams_of = jax.random.split(jax.random.key(seed), 2)
    return {
        "matrix": draw_matrix(jax.random.fold_in(streams_of[1], 71), 0),
    }


def reference(matrix):
    order = MR * N_ROW * B
    work = matrix.reshape(order, order)
    for k in range(STEPS):
        low = k * B
        high = low + B
        factor = jnp.linalg.cholesky(work[low:high, low:high])
        below = work[high:, low:high]
        solved = jax.scipy.linalg.solve_triangular(factor, below.T, lower=True).T
        update = jnp.dot(solved.astype(jnp.float32), solved.T.astype(jnp.float32), precision=lax.Precision.HIGHEST, preferred_element_type=jnp.float32)
        work = work.at[high:, high:].add(-update)
        work = work.at[:low, low:high].set(jnp.zeros((low, B), jnp.float32))
        work = work.at[low:high, low:high].set(factor)
        work = work.at[high:, low:high].set(solved)
    return work.reshape(matrix.shape)
```

```python
import jax, jax.numpy as jnp, functools
from jax import lax
from jax.experimental import pallas as pl
from jax.experimental.pallas import tpu as pltpu

F32, BF16 = jnp.float32, jnp.bfloat16

def over_lanes(v, c):
    return jnp.broadcast_to(v[:, c:c + 1], (8, 128))

def over_rows(v, r):
    return jnp.broadcast_to(v[r:r + 1, :], (8, 128))

def eliminate(rows):
    sub = lax.broadcasted_iota(jnp.int32, (8, 128), 0)
    rows = list(rows)
    diag = [over_lanes(rows[0], t) for t in range(8)]
    for s in range(8):
        off = {i: [over_lanes(rows[i], 8 * s + m) for m in range(8)] for i in range(s + 1, 8)}
        nxt = [over_lanes(rows[s + 1], 8 * (s + 1) + t) for t in range(8)] if s < 7 else None
        top = rows[s]
        for m in range(8):
            root = lax.rsqrt(over_rows(diag[m], m))
            lead = diag[m] * root
            unit = over_rows(top, m) * root
            top = jnp.where(sub == m, unit, top - jnp.where(sub > m, lead, 0.0) * unit)
            scal = {t: over_rows(lead, t) for t in range(m + 1, 8)}
            for t in range(m + 1, 8):
                diag[t] = diag[t] - lead * scal[t]
            for i in range(s + 1, 8):
                mult = off[i][m] * root
                for t in range(m + 1, 8):
                    off[i][t] = off[i][t] - mult * scal[t]
                rows[i] = rows[i] - mult * unit
                if i == s + 1:
                    for t in range(8):
                        nxt[t] = nxt[t] - mult * over_rows(mult, t)
        rows[s] = top
        diag = nxt
    return rows

def split(x):
    hi = x.astype(BF16)
    return hi, (x - hi.astype(F32)).astype(BF16)

def nt(a, b):
    return lax.dot_general(a, b, (((1,), (1,)), ((), ())), preferred_element_type=F32)

def nn(a, b):
    return lax.dot_general(a, b, (((1,), (0,)), ((), ())), preferred_element_type=F32)

def factor_tile(tb, ud, lb, zpad, w_hi, w_lo):
    low = lax.broadcasted_iota(jnp.int32, (64, 128), 1) < 64
    eye = jnp.where(
        lax.broadcasted_iota(jnp.int32, (64, 128), 1)
        == lax.broadcasted_iota(jnp.int32, (64, 128), 0) + 64, 1.0, 0.0).astype(F32)
    zpad[...] = jnp.zeros_like(zpad)

    def group(g, _):
        block = jnp.where(low, tb[g, g], eye)
        done = eliminate([block[8 * i:8 * i + 8] for i in range(8)])
        m = jnp.concatenate(done, 0)
        ud[g] = m
        wz = jnp.where(low, 0.0, m)
        wz_hi, wz_lo = split(wz)
        tcol = tb[:, g].reshape(256, 128)
        t_hi, t_lo = split(tcol)
        w2_hi = jnp.concatenate([wz_hi, wz_hi], 0)
        w2_lo = jnp.concatenate([wz_lo, wz_lo], 0)
        p = nt(jnp.concatenate([t_hi, t_lo], 1), jnp.concatenate([w2_hi, w2_hi], 1)) + nt(t_hi, w2_lo)
        rowblk = lax.broadcasted_iota(jnp.int32, (256, 128), 0) // 64
        p = jnp.where(rowblk > g, p, 0.0)
        lb[:, g] = p.reshape(4, 64, 128)
        hi = p.astype(BF16)
        hif = hi.astype(F32)
        lof = p - hif
        lo = lof.astype(BF16)
        lowp = lax.broadcasted_iota(jnp.int32, (256, 128), 1) < 64
        lhs = jnp.concatenate([jnp.where(lowp, hif, lof).astype(BF16),
                               jnp.where(lowp, hif, 0.0).astype(BF16)], 1)
        for h in range(2):
            parts = []
            for j in (2 * h, 2 * h + 1):
                pj = jnp.concatenate([hi[64 * j:64 * j + 64], lo[64 * j:64 * j + 64]], 1)
                parts += [pj, pj]
            upd = nt(lhs, jnp.concatenate(parts, 0))
            for j in range(2):
                tb[:, 2 * h + j] = tb[:, 2 * h + j] - upd[:, 128 * j:128 * j + 128].reshape(4, 64, 128)
        z = zpad[pl.ds(pl.multiple_of(64 * g, 64), 128), :]
        z_hi, z_lo = split(z)
        mix = nn(jnp.concatenate([wz_hi, wz_lo], 1), jnp.concatenate([z_hi, z_hi], 0)) + nn(wz_hi, z_lo)
        turned = pltpu.roll(m, 64, 1)
        both = jnp.where(low, turned, m)
        here = lax.broadcasted_iota(jnp.int32, (64, 256), 1) // 64 == g
        wrow = jnp.where(here, jnp.concatenate([both, both], 1), -mix)
        at = pl.ds(pl.multiple_of(64 * g, 64), 64)
        r_hi, r_lo = split(wrow)
        w_hi[at, :] = r_hi
        w_lo[at, :] = r_lo
        zpad[64:, :] = zpad[64:, :] + nn(lhs, jnp.concatenate([r_hi, r_hi, r_lo, r_lo], 0))
        return 0
    lax.fori_loop(0, 4, group, 0)

def blocks(tile, tb):
    low = lax.broadcasted_iota(jnp.int32, (256, 128), 1) < 64
    for h in range(2):
        x = tile[:, 128 * h:128 * h + 128]
        r = pltpu.roll(x, 64, 1)
        tb[:, 2 * h] = jnp.where(low, x, r).reshape(4, 64, 128)
        tb[:, 2 * h + 1] = jnp.where(low, r, x).reshape(4, 64, 128)


B = 256
STEPS = 8
SLOTS = 10

def nt3(ah, al, bh, bl):
    return nt(ah, bh) + nt(ah, bl) + nt(al, bh)

def nn3(ah, al, bh, bl):
    return nn(ah, bh) + nn(ah, bl) + nn(al, bh)

def local_kernel(p, q, d_ref, x_ref, y_ref, own_ref, out_ref,
                 g, lh, ll, uh, ul, y, tb, ud, lb, zpad, wh, wl, held, g_sem, y_sem):
    copies = []
    for k in range(STEPS):
        mine = [pltpu.make_async_copy(d_ref.at[k, i], g.at[k, i], g_sem.at[k, i]) for i in range(k, STEPS)]
        mine += [pltpu.make_async_copy(x_ref.at[k, a], g.at[k, STEPS + a], g_sem.at[k, STEPS + a]) for a in range(2)]
        mine += [pltpu.make_async_copy(y_ref.at[k], y.at[k], y_sem.at[k])]
        copies.append(mine)
        for c in mine:
            c.start()
    out_ref[...] = own_ref[...]

    def step(k, _):
        def arrive(i, _):
            pltpu.make_async_copy(d_ref.at[k, i], g.at[k, i], g_sem.at[k, i]).wait()
            return 0
        lax.fori_loop(k, STEPS, arrive, 0)
        for a in range(2):
            pltpu.make_async_copy(x_ref.at[k, a], g.at[k, STEPS + a], g_sem.at[k, STEPS + a]).wait()
        pltpu.make_async_copy(y_ref.at[k], y.at[k], y_sem.at[k]).wait()

        def pair(r):
            return pl.ds(2 * r, 2)

        def update(r, _):
            def term(m, _):
                got = nt3(lh[m, pair(r)].reshape(512, B), ll[m, pair(r)].reshape(512, B), lh[m, k], ll[m, k])
                g[k, pair(r)] = g[k, pair(r)] - got.reshape(2, B, B)
                return 0
            return lax.fori_loop(0, k, term, 0)
        lax.fori_loop(k // 2, 5, update, 0)

        blocks(g[k, k], tb)
        factor_tile(tb, ud, lb, zpad, wh, wl)

        def solve(r, _):
            ah, al = split(g[k, pair(r)].reshape(512, B))
            got = nt3(ah, al, wh[...], wl[...]).reshape(2, B, B)
            hi, lo = split(got)
            lh[k, pair(r)] = hi
            ll[k, pair(r)] = lo
            return 0
        lax.fori_loop(k // 2, 4, solve, 0)

        ah, al = split(g[k, 8:10].reshape(512, B))
        got = nt3(ah, al, wh[...], wl[...])
        got = jnp.concatenate([jnp.where(p > k, got[:B], 0.0), got[B:]], 0)
        hi, lo = split(got)
        lh[k, 8:10] = hi.reshape(2, B, B)
        ll[k, 8:10] = lo.reshape(2, B, B)

        @pl.when(q == k)
        def _():
            held[...] = got.reshape(2, B, B)

        @pl.when((q == k) & (p == k))
        def _():
            low = lax.broadcasted_iota(jnp.int32, (64, 128), 1) < 64
            tri = lax.broadcasted_iota(jnp.int32, (64, 128), 0) <= lax.broadcasted_iota(jnp.int32, (64, 128), 1)
            for i in range(4):
                up = jnp.where(tri & low, ud[i], 0.0)
                turned = jnp.concatenate([up, jnp.zeros((64, 128), F32)], 0).T[:64]
                twice = turned + pltpu.roll(turned, 64, 1)
                parts = [lb[i, j] if j < i else (twice if j == i else jnp.zeros((64, 128), F32)) for j in range(4)]
                for h in range(2):
                    held[0, 64 * i:64 * i + 64, 128 * h:128 * h + 128] = jnp.where(low, parts[2 * h], parts[2 * h + 1])

        def uterm(m, _):
            y[k] = y[k] - nn3(lh[m, k], ll[m, k], uh[m], ul[m])
            return 0
        lax.fori_loop(0, k, uterm, 0)
        yh, yl = split(y[k])
        u = nn3(wh[...], wl[...], yh, yl)
        u = jnp.concatenate([jnp.where(q > k, u[:, :B], 0.0), u[:, B:]], 1)
        hi, lo = split(u)
        uh[k] = hi
        ul[k] = lo
        for a in range(2):
            out_ref[a] = out_ref[a] - nn3(lh[k, 8 + a], ll[k, 8 + a], hi, lo)
        return 0
    lax.fori_loop(0, STEPS, step, 0)

    @pl.when(q < STEPS)
    def _():
        out_ref[:, :, :B] = held[...]

def scratch():
    V = pltpu.VMEM
    return [V((STEPS, SLOTS, B, B), F32), V((STEPS, SLOTS, B, B), BF16), V((STEPS, SLOTS, B, B), BF16),
            V((STEPS, B, 2 * B), BF16), V((STEPS, B, 2 * B), BF16), V((STEPS, B, 2 * B), F32),
            V((4, 4, 64, 128), F32), V((4, 64, 128), F32), V((4, 4, 64, 128), F32), V((320, B), F32),
            V((B, B), BF16), V((B, B), BF16), V((2, B, B), F32),
            pltpu.SemaphoreType.DMA((STEPS, SLOTS)), pltpu.SemaphoreType.DMA((STEPS,))]

from jax.sharding import PartitionSpec as P


def local_entry(*refs):
    local_kernel(lax.axis_index("row"), lax.axis_index("col"), *refs)


def on_device(matrix):
    own = matrix.reshape(2, B, 2 * B)
    x = lax.all_gather(own[:, :, :B], "col")
    y = lax.all_gather(own[0], "row")
    d = lax.all_gather(y[:STEPS, :, :B], "col")
    out = pl.pallas_call(
        local_entry,
        out_shape=jax.ShapeDtypeStruct((2, B, 2 * B), F32),
        in_specs=[pl.BlockSpec(memory_space=pl.ANY)] * 3 + [pl.BlockSpec(memory_space=pltpu.VMEM)],
        out_specs=pl.BlockSpec(memory_space=pltpu.VMEM),
        scratch_shapes=scratch(),
        compiler_params=pltpu.CompilerParams(vmem_limit_bytes=63 * 1024 * 1024),
    )(d, x, y, own)
    return out.reshape(matrix.shape)


def solution(mesh):
    spec = P(None, "row", None, None, "col", None)
    return jax.shard_map(on_device, mesh=mesh, in_specs=(spec,), out_specs=spec, check_vma=False)
```

```python
import jax, jax.numpy as jnp, functools
from jax import lax
from jax.experimental import pallas as pl
from jax.experimental.pallas import tpu as pltpu

F32, BF16 = jnp.float32, jnp.bfloat16

def over_lanes(v, c):
    return jnp.broadcast_to(v[:, c:c + 1], (8, 128))

def over_rows(v, r):
    return jnp.broadcast_to(v[r:r + 1, :], (8, 128))

def eliminate(rows):
    sub = lax.broadcasted_iota(jnp.int32, (8, 128), 0)
    rows = list(rows)
    diag = [over_lanes(rows[0], t) for t in range(8)]
    for s in range(8):
        off = {i: [over_lanes(rows[i], 8 * s + m) for m in range(8)] for i in range(s + 1, 8)}
        nxt = [over_lanes(rows[s + 1], 8 * (s + 1) + t) for t in range(8)] if s < 7 else None
        top = rows[s]
        for m in range(8):
            root = lax.rsqrt(over_rows(diag[m], m))
            lead = diag[m] * root
            unit = over_rows(top, m) * root
            top = jnp.where(sub == m, unit, top - jnp.where(sub > m, lead, 0.0) * unit)
            scal = {t: over_rows(lead, t) for t in range(m + 1, 8)}
            for t in range(m + 1, 8):
                diag[t] = diag[t] - lead * scal[t]
            for i in range(s + 1, 8):
                mult = off[i][m] * root
                for t in range(m + 1, 8):
                    off[i][t] = off[i][t] - mult * scal[t]
                rows[i] = rows[i] - mult * unit
                if i == s + 1:
                    for t in range(8):
                        nxt[t] = nxt[t] - mult * over_rows(mult, t)
        rows[s] = top
        diag = nxt
    return rows

def split(x):
    hi = x.astype(BF16)
    return hi, (x - hi.astype(F32)).astype(BF16)

def nt(a, b):
    return lax.dot_general(a, b, (((1,), (1,)), ((), ())), preferred_element_type=F32)

def nn(a, b):
    return lax.dot_general(a, b, (((1,), (0,)), ((), ())), preferred_element_type=F32)

def factor_tile(tb, ud, lb, zpad, w_hi, w_lo):
    low = lax.broadcasted_iota(jnp.int32, (64, 128), 1) < 64
    eye = jnp.where(
        lax.broadcasted_iota(jnp.int32, (64, 128), 1)
        == lax.broadcasted_iota(jnp.int32, (64, 128), 0) + 64, 1.0, 0.0).astype(F32)
    zpad[...] = jnp.zeros_like(zpad)

    def group(g, _):
        block = jnp.where(low, tb[g, g], eye)
        done = eliminate([block[8 * i:8 * i + 8] for i in range(8)])
        m = jnp.concatenate(done, 0)
        ud[g] = m
        wz = jnp.where(low, 0.0, m)
        wz_hi, wz_lo = split(wz)
        tcol = tb[:, g].reshape(256, 128)
        t_hi, t_lo = split(tcol)
        w2_hi = jnp.concatenate([wz_hi, wz_hi], 0)
        w2_lo = jnp.concatenate([wz_lo, wz_lo], 0)
        p = nt(jnp.concatenate([t_hi, t_lo], 1), jnp.concatenate([w2_hi, w2_hi], 1)) + nt(t_hi, w2_lo)
        rowblk = lax.broadcasted_iota(jnp.int32, (256, 128), 0) // 64
        p = jnp.where(rowblk > g, p, 0.0)
        lb[:, g] = p.reshape(4, 64, 128)
        hi = p.astype(BF16)
        hif = hi.astype(F32)
        lof = p - hif
        lo = lof.astype(BF16)
        lowp = lax.broadcasted_iota(jnp.int32, (256, 128), 1) < 64
        lhs = jnp.concatenate([jnp.where(lowp, hif, lof).astype(BF16),
                               jnp.where(lowp, hif, 0.0).astype(BF16)], 1)
        for h in range(2):
            parts = []
            for j in (2 * h, 2 * h + 1):
                pj = jnp.concatenate([hi[64 * j:64 * j + 64], lo[64 * j:64 * j + 64]], 1)
                parts += [pj, pj]
            upd = nt(lhs, jnp.concatenate(parts, 0))
            for j in range(2):
                tb[:, 2 * h + j] = tb[:, 2 * h + j] - upd[:, 128 * j:128 * j + 128].reshape(4, 64, 128)
        z = zpad[pl.ds(pl.multiple_of(64 * g, 64), 128), :]
        z_hi, z_lo = split(z)
        mix = nn(jnp.concatenate([wz_hi, wz_lo], 1), jnp.concatenate([z_hi, z_hi], 0)) + nn(wz_hi, z_lo)
        turned = pltpu.roll(m, 64, 1)
        both = jnp.where(low, turned, m)
        here = lax.broadcasted_iota(jnp.int32, (64, 256), 1) // 64 == g
        wrow = jnp.where(here, jnp.concatenate([both, both], 1), -mix)
        at = pl.ds(pl.multiple_of(64 * g, 64), 64)
        r_hi, r_lo = split(wrow)
        w_hi[at, :] = r_hi
        w_lo[at, :] = r_lo
        zpad[64:, :] = zpad[64:, :] + nn(lhs, jnp.concatenate([r_hi, r_hi, r_lo, r_lo], 0))
        return 0
    lax.fori_loop(0, 4, group, 0)

def blocks(tile, tb):
    low = lax.broadcasted_iota(jnp.int32, (256, 128), 1) < 64
    for h in range(2):
        x = tile[:, 128 * h:128 * h + 128]
        r = pltpu.roll(x, 64, 1)
        tb[:, 2 * h] = jnp.where(low, x, r).reshape(4, 64, 128)
        tb[:, 2 * h + 1] = jnp.where(low, r, x).reshape(4, 64, 128)


B = 256
STEPS = 8
SLOTS = 10

def nt3(ah, al, bh, bl):
    return nt(ah, bh) + nt(ah, bl) + nt(al, bh)

def nn3(ah, al, bh, bl):
    return nn(ah, bh) + nn(ah, bl) + nn(al, bh)

def local_kernel(p, q, g_in, y_in, own_ref, out_ref,
                 g, lh, ll, uh, ul, y, tb, ud, lb, zpad, wh, wl, held, g_sem, y_sem):
    def slot_of(i):
        return jnp.where((i == p) & (i < STEPS), STEPS, i)

    for k in range(STEPS):
        for i in range(k, SLOTS):
            pltpu.make_async_copy(g_in.at[k, slot_of(i)], g.at[k, i], g_sem.at[k, i]).start()
        pltpu.make_async_copy(y_in.at[k], y.at[k], y_sem.at[k]).start()
    out_ref[...] = own_ref[...]

    def step(k, _):
        def arrive(i, _):
            pltpu.make_async_copy(g_in.at[k, i], g.at[k, i], g_sem.at[k, i]).wait()
            return 0
        lax.fori_loop(k, SLOTS, arrive, 0)
        pltpu.make_async_copy(y_in.at[k], y.at[k], y_sem.at[k]).wait()

        def pair(r):
            return pl.ds(2 * r, 2)

        def update(r, _):
            def term(m, _):
                got = nt3(lh[m, pair(r)].reshape(512, B), ll[m, pair(r)].reshape(512, B), lh[m, k], ll[m, k])
                g[k, pair(r)] = g[k, pair(r)] - got.reshape(2, B, B)
                return 0
            return lax.fori_loop(0, k, term, 0)
        lax.fori_loop(k // 2, 5, update, 0)

        blocks(g[k, k], tb)
        factor_tile(tb, ud, lb, zpad, wh, wl)

        def solve(r, _):
            ah, al = split(g[k, pair(r)].reshape(512, B))
            got = nt3(ah, al, wh[...], wl[...]).reshape(2, B, B)
            hi, lo = split(got)
            lh[k, pair(r)] = hi
            ll[k, pair(r)] = lo
            return 0
        lax.fori_loop(k // 2, 4, solve, 0)

        ah, al = split(g[k, 8:10].reshape(512, B))
        got = nt3(ah, al, wh[...], wl[...])
        got = jnp.concatenate([jnp.where(p > k, got[:B], 0.0), got[B:]], 0)
        hi, lo = split(got)
        lh[k, 8:10] = hi.reshape(2, B, B)
        ll[k, 8:10] = lo.reshape(2, B, B)

        @pl.when(q == k)
        def _():
            held[...] = got.reshape(2, B, B)

        @pl.when((q == k) & (p == k))
        def _():
            low = lax.broadcasted_iota(jnp.int32, (64, 128), 1) < 64
            tri = lax.broadcasted_iota(jnp.int32, (64, 128), 0) <= lax.broadcasted_iota(jnp.int32, (64, 128), 1)
            for i in range(4):
                up = jnp.where(tri & low, ud[i], 0.0)
                turned = jnp.concatenate([up, jnp.zeros((64, 128), F32)], 0).T[:64]
                twice = turned + pltpu.roll(turned, 64, 1)
                parts = [lb[i, j] if j < i else (twice if j == i else jnp.zeros((64, 128), F32)) for j in range(4)]
                for h in range(2):
                    held[0, 64 * i:64 * i + 64, 128 * h:128 * h + 128] = jnp.where(low, parts[2 * h], parts[2 * h + 1])

        def uterm(m, _):
            y[k] = y[k] - nn3(lh[m, k], ll[m, k], uh[m], ul[m])
            return 0
        lax.fori_loop(0, k, uterm, 0)
        yh, yl = split(y[k])
        u = nn3(wh[...], wl[...], yh, yl)
        u = jnp.concatenate([jnp.where(q > k, u[:, :B], 0.0), u[:, B:]], 1)
        hi, lo = split(u)
        uh[k] = hi
        ul[k] = lo
        for a in range(2):
            out_ref[a] = out_ref[a] - nn3(lh[k, 8 + a], ll[k, 8 + a], hi, lo)
        return 0
    lax.fori_loop(0, STEPS, step, 0)

    @pl.when(q < STEPS)
    def _():
        out_ref[:, :, :B] = held[...]

def scratch():
    V = pltpu.VMEM
    return [V((STEPS, SLOTS, B, B), F32), V((STEPS, SLOTS, B, B), BF16), V((STEPS, SLOTS, B, B), BF16),
            V((STEPS, B, 2 * B), BF16), V((STEPS, B, 2 * B), BF16), V((STEPS, B, 2 * B), F32),
            V((4, 4, 64, 128), F32), V((4, 64, 128), F32), V((4, 4, 64, 128), F32), V((320, B), F32),
            V((B, B), BF16), V((B, B), BF16), V((2, B, B), F32),
            pltpu.SemaphoreType.DMA((STEPS, SLOTS)), pltpu.SemaphoreType.DMA((STEPS,))]
MESH = pl.DeviceIdType.MESH

class Comm:
    def __init__(self, p, q, own, g, y, send_sem, g_sem, y_sem, x_sem, d_sem, own_sem):
        self.p, self.q, self.own, self.g, self.y = p, q, own, g, y
        self.px, self.py, self.pz, self.c = p % 4, p // 4, q // 2, q % 2
        self.send_sem, self.g_sem, self.y_sem = send_sem, g_sem, y_sem
        self.x_sem, self.d_sem, self.own_sem = x_sem, d_sem, own_sem
        self.sent = []

    def at_z(self, d):
        return (self.p, 2 * ((self.pz + d) % 8) + self.c)

    def at_y(self, d):
        return (4 * ((self.py + d) % 4) + self.px, self.q)

    def at_x(self, d):
        return (4 * self.py + (self.px + d) % 4, self.q)

    def sibling(self):
        return (self.p, 2 * self.pz + 1 - self.c)

    def barrier(self):
        b = pltpu.get_barrier_semaphore()
        peers = [self.at_z(1), self.at_z(-1), self.at_y(1), self.at_y(-1), self.at_x(1), self.at_x(-1), self.sibling()]
        for d in peers:
            pl.semaphore_signal(b, inc=1, device_id=d, device_id_type=MESH)
        pl.semaphore_wait(b, len(peers))

    def send(self, cond, src, dst, sem, to):
        c = pltpu.make_async_remote_copy(src_ref=src, dst_ref=dst, send_sem=self.send_sem.at[len(self.sent)],
                                         recv_sem=sem, device_id=to, device_id_type=MESH)
        pl.when(cond)(c.start)
        self.sent.append((cond, c))

    def take(self, cond, ref, sem):
        c = pltpu.make_async_remote_copy(src_ref=ref, dst_ref=ref, send_sem=self.send_sem.at[0],
                                         recv_sem=sem, device_id=self.sibling(), device_id_type=MESH)
        pl.when(cond)(c.wait_recv)

    def drain(self):
        for cond, c in self.sent:
            pl.when(cond)(c.wait_send)

    def local(self):
        p, q = self.p, self.q
        lead = jnp.minimum(q, 7)
        rowk = jnp.minimum(p, 7)
        return [(q < 8, pltpu.make_async_copy(self.own.at[a, :, pl.ds(0, B)], self.g.at[lead, 8 + a], self.own_sem.at[a]))
                for a in range(2)] + [
            (p < 8, pltpu.make_async_copy(self.own.at[0], self.y.at[rowk], self.own_sem.at[2]))]

    def gp(self, k, slot, piece):
        return self.g.at[k, slot, pl.ds(64 * piece, 64)]

    def z_hop(self, s):
        for d, pieces in ((1, (0, 1)), (-1, (2, 3))):
            zs = (self.pz - d * s) % 8
            on = zs < 4
            k = jnp.minimum(2 * zs + self.c, 7)
            for a in range(2):
                for piece in pieces:
                    ref, sem = self.gp(k, 8 + a, piece), self.g_sem.at[k, 8 + a, piece]
                    if s > 0:
                        self.take(on, ref, sem)
                    if s < 7:
                        self.send(on, ref, ref, sem, self.at_z(d))
                    if a == 0:
                        row = on & (self.p < 8) & (k <= self.p)
                        pp = jnp.minimum(self.p, 7)
                        for e in (1, -1):
                            self.send(row, ref, self.gp(k, pp, piece), self.g_sem.at[k, pp, piece], self.at_y(e))

    def y_own(self):
        pp = jnp.minimum(self.p, 7)
        for piece in range(4):
            ref = self.y.at[pp, pl.ds(64 * piece, 64)]
            for e in (1, -1):
                self.send(self.p < 8, ref, ref, self.y_sem.at[pp, piece], self.at_y(e))

    def item(self, k):
        if k is None:
            ref = lambda r, piece: self.y.at[r, pl.ds(64 * piece, 64)]
            return ref, ref, (lambda r, piece: self.y_sem.at[r, piece]), (lambda r: True)
        return ((lambda r, piece: self.gp(k, jnp.where(r == self.p, 8, r), piece)),
                (lambda r, piece: self.gp(k, r, piece)),
                (lambda r, piece: self.g_sem.at[k, r, piece]),
                (lambda r: k <= r))

    def y_forward(self, k):
        src, dst, sem, has = self.item(k)
        for d, pieces in ((1, (0, 1)), (-1, (2, 3))):
            ys = (self.py - d) % 4
            r = jnp.minimum(4 * ys + self.px, 7)
            on = (ys < 2) & has(r)
            for piece in pieces:
                self.take(on, dst(r, piece), sem(r, piece))
                self.send(on, dst(r, piece), dst(r, piece), sem(r, piece), self.at_y(d))

    def x_send(self, k):
        src, dst, sem, has = self.item(k)
        for ys in range(2):
            r = 4 * ys + self.px
            dist = (self.py - ys) % 4
            for piece in range(4):
                rest = (dist == 2) | (dist == (1 if piece >= 2 else 3))
                self.take(rest & has(r), dst(r, piece), sem(r, piece))
                for e in (1, -1):
                    self.send(jnp.bool_(True) & has(r), src(r, piece), dst(r, piece), sem(r, piece), self.at_x(e))
            if k is not None:
                self.send(has(r) & (dist != 0), self.g.at[k, r], self.g.at[k, r], self.d_sem.at[k, r], self.sibling())

    def x_forward(self, k):
        src, dst, sem, has = self.item(k)
        for d, pieces in ((1, (0, 1)), (-1, (2, 3))):
            xs = (self.px - d) % 4
            for ys in range(2):
                r = 4 * ys + xs
                for piece in pieces:
                    self.take(jnp.bool_(True) & has(r), dst(r, piece), sem(r, piece))
                    self.send(jnp.bool_(True) & has(r), dst(r, piece), dst(r, piece), sem(r, piece), self.at_x(d))

    def finish(self, k):
        src, dst, sem, has = self.item(k)
        for dx in (1, 3, 2):
            xs = (self.px - dx) % 4
            pieces = {1: (2, 3), 3: (0, 1), 2: (0, 1, 2, 3)}[dx]
            for ys in range(2):
                r = 4 * ys + xs
                for piece in pieces:
                    self.take(jnp.bool_(True) & has(r), dst(r, piece), sem(r, piece))
                if k is not None:
                    self.send(has(r), self.g.at[k, r], self.g.at[k, r], self.d_sem.at[k, r], self.sibling())

    def x_sibling(self):
        for i in range(4):
            k = 2 * i + self.c
            self.send(jnp.bool_(True) & (k < 8), self.g.at[k, pl.ds(8, 2)], self.g.at[k, pl.ds(8, 2)], self.x_sem.at[k], self.sibling())

    def from_sibling(self):
        for i in range(4):
            k = 2 * i + 1 - self.c
            self.take(k < 8, self.g.at[k, pl.ds(8, 2)], self.x_sem.at[k])
            for r in range(8):
                self.take((k <= r) & (r != self.p), self.g.at[k, r], self.d_sem.at[k, r])

    def run(self):
        mine = self.local()
        for on, c in mine:
            pl.when(on)(c.start)
        self.barrier()
        for on, c in mine:
            pl.when(on)(c.wait)
        ks = [2 * i + self.c for i in range(4)]
        self.z_hop(0)
        self.y_own()
        self.z_hop(1)
        self.z_hop(2)
        self.y_forward(None)
        self.z_hop(3)
        self.x_send(None)
        self.z_hop(4)
        self.x_forward(None)
        self.z_hop(5)
        self.z_hop(6)
        self.z_hop(7)
        self.x_sibling()
        for k in ks:
            self.y_forward(k)
        for k in ks:
            self.x_send(k)
        for k in ks:
            self.x_forward(k)
        for k in ks:
            self.finish(k)
        self.finish(None)
        self.from_sibling()
        self.drain()

N_SEND = 640

def comm_scratch():
    D = pltpu.SemaphoreType.DMA
    return [D((N_SEND,)), D((8, 10, 4)), D((8, 4)), D((8,)), D((8, 8)), D((3,))]

from jax.sharding import PartitionSpec as P


def gather_entry(own, g_out, y_out, g, y, out_sem, *sems):
    p, q = lax.axis_index("row"), lax.axis_index("col")
    Comm(p, q, own, g, y, *sems).run()
    outs = [pltpu.make_async_copy(y, y_out, out_sem.at[0])]
    for k in range(8):
        outs.append(pltpu.make_async_copy(g.at[k, pl.ds(k, 10 - k)], g_out.at[k, pl.ds(k, 10 - k)], out_sem.at[1 + k]))

    row = jnp.minimum(p, 7)
    for c in outs:
        c.start()
    for c in outs:
        c.wait()


def local_entry(g_in, y_in, own_ref, out_ref, *rest):
    local_kernel(lax.axis_index("row"), lax.axis_index("col"), g_in, y_in, own_ref, out_ref, *rest)


def on_device(matrix):
    own = matrix.reshape(2, B, 2 * B)
    any_spec = pl.BlockSpec(memory_space=pl.ANY)
    g, y = pl.pallas_call(
        gather_entry,
        out_shape=[jax.ShapeDtypeStruct((STEPS, SLOTS, B, B), F32), jax.ShapeDtypeStruct((STEPS, B, 2 * B), F32)],
        in_specs=[any_spec],
        out_specs=[any_spec] * 2,
        scratch_shapes=[pltpu.VMEM((STEPS, SLOTS, B, B), F32), pltpu.VMEM((STEPS, B, 2 * B), F32),
                        pltpu.SemaphoreType.DMA((9,))] + comm_scratch(),
        compiler_params=pltpu.CompilerParams(vmem_limit_bytes=63 * 1024 * 1024, collective_id=0, has_side_effects=True),
        name="gather",
    )(own)
    out = pl.pallas_call(
        local_entry,
        out_shape=jax.ShapeDtypeStruct((2, B, 2 * B), F32),
        in_specs=[any_spec] * 2 + [pl.BlockSpec(memory_space=pltpu.VMEM)],
        out_specs=pl.BlockSpec(memory_space=pltpu.VMEM),
        scratch_shapes=scratch(),
        compiler_params=pltpu.CompilerParams(vmem_limit_bytes=63 * 1024 * 1024),
        name="local",
    )(g, y, own)
    return out.reshape(matrix.shape)


def solution(mesh):
    spec = P(None, "row", None, None, "col", None)
    return jax.shard_map(on_device, mesh=mesh, in_specs=(spec,), out_specs=spec, check_vma=False)
```

```python
import jax, jax.numpy as jnp, functools
from jax import lax
from jax.experimental import pallas as pl
from jax.experimental.pallas import tpu as pltpu

F32, BF16 = jnp.float32, jnp.bfloat16

def over_lanes(v, c):
    return jnp.broadcast_to(v[:, c:c + 1], (8, 128))

def over_rows(v, r):
    return jnp.broadcast_to(v[r:r + 1, :], (8, 128))

def eliminate(rows):
    sub = lax.broadcasted_iota(jnp.int32, (8, 128), 0)
    rows = list(rows)
    diag = [over_lanes(rows[0], t) for t in range(8)]
    for s in range(8):
        off = {i: [over_lanes(rows[i], 8 * s + m) for m in range(8)] for i in range(s + 1, 8)}
        nxt = [over_lanes(rows[s + 1], 8 * (s + 1) + t) for t in range(8)] if s < 7 else None
        top = rows[s]
        for m in range(8):
            root = lax.rsqrt(over_rows(diag[m], m))
            lead = diag[m] * root
            unit = over_rows(top, m) * root
            top = jnp.where(sub == m, unit, top - jnp.where(sub > m, lead, 0.0) * unit)
            scal = {t: over_rows(lead, t) for t in range(m + 1, 8)}
            for t in range(m + 1, 8):
                diag[t] = diag[t] - lead * scal[t]
            for i in range(s + 1, 8):
                mult = off[i][m] * root
                for t in range(m + 1, 8):
                    off[i][t] = off[i][t] - mult * scal[t]
                rows[i] = rows[i] - mult * unit
                if i == s + 1:
                    for t in range(8):
                        nxt[t] = nxt[t] - mult * over_rows(mult, t)
        rows[s] = top
        diag = nxt
    return rows

def split(x):
    hi = x.astype(BF16)
    return hi, (x - hi.astype(F32)).astype(BF16)

def nt(a, b):
    return lax.dot_general(a, b, (((1,), (1,)), ((), ())), preferred_element_type=F32)

def nn(a, b):
    return lax.dot_general(a, b, (((1,), (0,)), ((), ())), preferred_element_type=F32)

def factor_tile(tb, ud, lb, zpad, w_hi, w_lo):
    low = lax.broadcasted_iota(jnp.int32, (64, 128), 1) < 64
    eye = jnp.where(
        lax.broadcasted_iota(jnp.int32, (64, 128), 1)
        == lax.broadcasted_iota(jnp.int32, (64, 128), 0) + 64, 1.0, 0.0).astype(F32)
    zpad[...] = jnp.zeros_like(zpad)

    def group(g, _):
        block = jnp.where(low, tb[g, g], eye)
        done = eliminate([block[8 * i:8 * i + 8] for i in range(8)])
        m = jnp.concatenate(done, 0)
        ud[g] = m
        wz = jnp.where(low, 0.0, m)
        wz_hi, wz_lo = split(wz)
        tcol = tb[:, g].reshape(256, 128)
        t_hi, t_lo = split(tcol)
        w2_hi = jnp.concatenate([wz_hi, wz_hi], 0)
        w2_lo = jnp.concatenate([wz_lo, wz_lo], 0)
        p = nt(jnp.concatenate([t_hi, t_lo], 1), jnp.concatenate([w2_hi, w2_hi], 1)) + nt(t_hi, w2_lo)
        rowblk = lax.broadcasted_iota(jnp.int32, (256, 128), 0) // 64
        p = jnp.where(rowblk > g, p, 0.0)
        lb[:, g] = p.reshape(4, 64, 128)
        hi = p.astype(BF16)
        hif = hi.astype(F32)
        lof = p - hif
        lo = lof.astype(BF16)
        lowp = lax.broadcasted_iota(jnp.int32, (256, 128), 1) < 64
        lhs = jnp.concatenate([jnp.where(lowp, hif, lof).astype(BF16),
                               jnp.where(lowp, hif, 0.0).astype(BF16)], 1)
        for h in range(2):
            parts = []
            for j in (2 * h, 2 * h + 1):
                pj = jnp.concatenate([hi[64 * j:64 * j + 64], lo[64 * j:64 * j + 64]], 1)
                parts += [pj, pj]
            upd = nt(lhs, jnp.concatenate(parts, 0))
            for j in range(2):
                tb[:, 2 * h + j] = tb[:, 2 * h + j] - upd[:, 128 * j:128 * j + 128].reshape(4, 64, 128)
        z = zpad[pl.ds(pl.multiple_of(64 * g, 64), 128), :]
        z_hi, z_lo = split(z)
        mix = nn(jnp.concatenate([wz_hi, wz_lo], 1), jnp.concatenate([z_hi, z_hi], 0)) + nn(wz_hi, z_lo)
        turned = pltpu.roll(m, 64, 1)
        both = jnp.where(low, turned, m)
        here = lax.broadcasted_iota(jnp.int32, (64, 256), 1) // 64 == g
        wrow = jnp.where(here, jnp.concatenate([both, both], 1), -mix)
        at = pl.ds(pl.multiple_of(64 * g, 64), 64)
        r_hi, r_lo = split(wrow)
        w_hi[at, :] = r_hi
        w_lo[at, :] = r_lo
        zpad[64:, :] = zpad[64:, :] + nn(lhs, jnp.concatenate([r_hi, r_hi, r_lo, r_lo], 0))
        return 0
    lax.fori_loop(0, 4, group, 0)

def blocks(tile, tb):
    low = lax.broadcasted_iota(jnp.int32, (256, 128), 1) < 64
    for h in range(2):
        x = tile[:, 128 * h:128 * h + 128]
        r = pltpu.roll(x, 64, 1)
        tb[:, 2 * h] = jnp.where(low, x, r).reshape(4, 64, 128)
        tb[:, 2 * h + 1] = jnp.where(low, r, x).reshape(4, 64, 128)


B = 256
STEPS = 8
SLOTS = 10

def nt3(ah, al, bh, bl):
    return nt(ah, bh) + nt(ah, bl) + nt(al, bh)

def nn3(ah, al, bh, bl):
    return nn(ah, bh) + nn(ah, bl) + nn(al, bh)

def compute(p, q, g, y, out_ref, lh, ll, uh, ul, tb, ud, lb, zpad, wh, wl, held):
    def step(k, _):
        def pair(r):
            return pl.ds(2 * r, 2)

        def update(r, _):
            def term(m, _):
                got = nt3(lh[m, pair(r)].reshape(512, B), ll[m, pair(r)].reshape(512, B), lh[m, k], ll[m, k])
                g[k, pair(r)] = g[k, pair(r)] - got.reshape(2, B, B)
                return 0
            return lax.fori_loop(0, k, term, 0)
        lax.fori_loop(k // 2, 5, update, 0)

        blocks(g[k, k], tb)
        factor_tile(tb, ud, lb, zpad, wh, wl)

        def solve(r, _):
            ah, al = split(g[k, pair(r)].reshape(512, B))
            got = nt3(ah, al, wh[...], wl[...]).reshape(2, B, B)
            hi, lo = split(got)
            lh[k, pair(r)] = hi
            ll[k, pair(r)] = lo
            return 0
        lax.fori_loop(k // 2, 4, solve, 0)

        ah, al = split(g[k, 8:10].reshape(512, B))
        got = nt3(ah, al, wh[...], wl[...])
        got = jnp.concatenate([jnp.where(p > k, got[:B], 0.0), got[B:]], 0)
        hi, lo = split(got)
        lh[k, 8:10] = hi.reshape(2, B, B)
        ll[k, 8:10] = lo.reshape(2, B, B)

        @pl.when(q == k)
        def _():
            held[...] = got.reshape(2, B, B)

        @pl.when((q == k) & (p == k))
        def _():
            low = lax.broadcasted_iota(jnp.int32, (64, 128), 1) < 64
            tri = lax.broadcasted_iota(jnp.int32, (64, 128), 0) <= lax.broadcasted_iota(jnp.int32, (64, 128), 1)
            for i in range(4):
                up = jnp.where(tri & low, ud[i], 0.0)
                turned = jnp.concatenate([up, jnp.zeros((64, 128), F32)], 0).T[:64]
                twice = turned + pltpu.roll(turned, 64, 1)
                parts = [lb[i, j] if j < i else (twice if j == i else jnp.zeros((64, 128), F32)) for j in range(4)]
                for h in range(2):
                    held[0, 64 * i:64 * i + 64, 128 * h:128 * h + 128] = jnp.where(low, parts[2 * h], parts[2 * h + 1])

        def uterm(m, _):
            y[k] = y[k] - nn3(lh[m, k], ll[m, k], uh[m], ul[m])
            return 0
        lax.fori_loop(0, k, uterm, 0)
        yh, yl = split(y[k])
        u = nn3(wh[...], wl[...], yh, yl)
        u = jnp.concatenate([jnp.where(q > k, u[:, :B], 0.0), u[:, B:]], 1)
        hi, lo = split(u)
        uh[k] = hi
        ul[k] = lo
        for a in range(2):
            out_ref[a] = out_ref[a] - nn3(lh[k, 8 + a], ll[k, 8 + a], hi, lo)
        return 0
    lax.fori_loop(0, STEPS, step, 0)

    @pl.when(q < STEPS)
    def _():
        out_ref[:, :, :B] = held[...]

def scratch():
    V = pltpu.VMEM
    return [V((STEPS, SLOTS, B, B), BF16), V((STEPS, SLOTS, B, B), BF16),
            V((STEPS, B, 2 * B), BF16), V((STEPS, B, 2 * B), BF16),
            V((4, 4, 64, 128), F32), V((4, 64, 128), F32), V((4, 4, 64, 128), F32), V((320, B), F32),
            V((B, B), BF16), V((B, B), BF16), V((2, B, B), F32)]
MESH = pl.DeviceIdType.MESH

class Comm:
    def __init__(self, p, q, own, g, y, send_sem, g_sem, y_sem, x_sem, d_sem, own_sem):
        self.p, self.q, self.own, self.g, self.y = p, q, own, g, y
        self.px, self.py, self.pz, self.c = p % 4, p // 4, q // 2, q % 2
        self.send_sem, self.g_sem, self.y_sem = send_sem, g_sem, y_sem
        self.x_sem, self.d_sem, self.own_sem = x_sem, d_sem, own_sem
        self.sent = []

    def at_z(self, d):
        return (self.p, 2 * ((self.pz + d) % 8) + self.c)

    def at_y(self, d):
        return (4 * ((self.py + d) % 4) + self.px, self.q)

    def at_x(self, d):
        return (4 * self.py + (self.px + d) % 4, self.q)

    def sibling(self):
        return (self.p, 2 * self.pz + 1 - self.c)

    def barrier(self):
        b = pltpu.get_barrier_semaphore()
        peers = [self.at_z(1), self.at_z(-1), self.at_y(1), self.at_y(-1), self.at_x(1), self.at_x(-1), self.sibling()]
        for d in peers:
            pl.semaphore_signal(b, inc=1, device_id=d, device_id_type=MESH)
        pl.semaphore_wait(b, len(peers))

    def send(self, cond, src, dst, sem, to):
        c = pltpu.make_async_remote_copy(src_ref=src, dst_ref=dst, send_sem=self.send_sem.at[len(self.sent)],
                                         recv_sem=sem, device_id=to, device_id_type=MESH)
        pl.when(cond)(c.start)
        self.sent.append((cond, c))

    def take(self, cond, ref, sem):
        c = pltpu.make_async_remote_copy(src_ref=ref, dst_ref=ref, send_sem=self.send_sem.at[0],
                                         recv_sem=sem, device_id=self.sibling(), device_id_type=MESH)
        pl.when(cond)(c.wait_recv)

    def drain(self):
        for cond, c in self.sent:
            pl.when(cond)(c.wait_send)

    def local(self):
        p, q = self.p, self.q
        lead = jnp.minimum(q, 7)
        rowk = jnp.minimum(p, 7)
        return [(q < 8, pltpu.make_async_copy(self.own.at[a, :, pl.ds(0, B)], self.g.at[lead, 8 + a], self.own_sem.at[a]))
                for a in range(2)] + [
            (p < 8, pltpu.make_async_copy(self.own.at[0], self.y.at[rowk], self.own_sem.at[2]))]

    def gp(self, k, slot, piece):
        return self.g.at[k, slot, pl.ds(64 * piece, 64)]

    def z_hop(self, s):
        for d, pieces in ((1, (0, 1)), (-1, (2, 3))):
            zs = (self.pz - d * s) % 8
            on = zs < 4
            k = jnp.minimum(2 * zs + self.c, 7)
            for a in range(2):
                for piece in pieces:
                    ref, sem = self.gp(k, 8 + a, piece), self.g_sem.at[k, 8 + a, piece]
                    if s > 0:
                        self.take(on, ref, sem)
                    if s < 7:
                        self.send(on, ref, ref, sem, self.at_z(d))
                    if a == 0:
                        row = on & (self.p < 8) & (k <= self.p)
                        pp = jnp.minimum(self.p, 7)
                        for e in (1, -1):
                            self.send(row, ref, self.gp(k, pp, piece), self.g_sem.at[k, pp, piece], self.at_y(e))

    def y_own(self):
        pp = jnp.minimum(self.p, 7)
        for piece in range(4):
            ref = self.y.at[pp, pl.ds(64 * piece, 64)]
            for e in (1, -1):
                self.send(self.p < 8, ref, ref, self.y_sem.at[pp, piece], self.at_y(e))

    def item(self, k):
        if k is None:
            ref = lambda r, piece: self.y.at[r, pl.ds(64 * piece, 64)]
            return ref, ref, (lambda r, piece: self.y_sem.at[r, piece]), (lambda r: True)
        return ((lambda r, piece: self.gp(k, jnp.where(r == self.p, 8, r), piece)),
                (lambda r, piece: self.gp(k, r, piece)),
                (lambda r, piece: self.g_sem.at[k, r, piece]),
                (lambda r: k <= r))

    def y_forward(self, k):
        src, dst, sem, has = self.item(k)
        for d, pieces in ((1, (0, 1)), (-1, (2, 3))):
            ys = (self.py - d) % 4
            r = jnp.minimum(4 * ys + self.px, 7)
            on = (ys < 2) & has(r)
            for piece in pieces:
                self.take(on, dst(r, piece), sem(r, piece))
                self.send(on, dst(r, piece), dst(r, piece), sem(r, piece), self.at_y(d))

    def x_send(self, k):
        src, dst, sem, has = self.item(k)
        for ys in range(2):
            r = 4 * ys + self.px
            dist = (self.py - ys) % 4
            for piece in range(4):
                rest = (dist == 2) | (dist == (1 if piece >= 2 else 3))
                self.take(rest & has(r), dst(r, piece), sem(r, piece))
                for e in (1, -1):
                    self.send(jnp.bool_(True) & has(r), src(r, piece), dst(r, piece), sem(r, piece), self.at_x(e))
            if k is not None:
                self.send(has(r) & (dist != 0), self.g.at[k, r], self.g.at[k, r], self.d_sem.at[k, r], self.sibling())

    def x_forward(self, k):
        src, dst, sem, has = self.item(k)
        for d, pieces in ((1, (0, 1)), (-1, (2, 3))):
            xs = (self.px - d) % 4
            for ys in range(2):
                r = 4 * ys + xs
                for piece in pieces:
                    self.take(jnp.bool_(True) & has(r), dst(r, piece), sem(r, piece))
                    self.send(jnp.bool_(True) & has(r), dst(r, piece), dst(r, piece), sem(r, piece), self.at_x(d))

    def finish(self, k):
        src, dst, sem, has = self.item(k)
        for dx in (1, 3, 2):
            xs = (self.px - dx) % 4
            pieces = {1: (2, 3), 3: (0, 1), 2: (0, 1, 2, 3)}[dx]
            for ys in range(2):
                r = 4 * ys + xs
                for piece in pieces:
                    self.take(jnp.bool_(True) & has(r), dst(r, piece), sem(r, piece))
                if k is not None:
                    self.send(has(r), self.g.at[k, r], self.g.at[k, r], self.d_sem.at[k, r], self.sibling())

    def x_sibling(self):
        for i in range(4):
            k = 2 * i + self.c
            self.send(jnp.bool_(True) & (k < 8), self.g.at[k, pl.ds(8, 2)], self.g.at[k, pl.ds(8, 2)], self.x_sem.at[k], self.sibling())

    def from_sibling(self):
        for i in range(4):
            k = 2 * i + 1 - self.c
            self.take(k < 8, self.g.at[k, pl.ds(8, 2)], self.x_sem.at[k])
            for r in range(8):
                self.take((k <= r) & (r != self.p), self.g.at[k, r], self.d_sem.at[k, r])

    def run(self):
        mine = self.local()
        for on, c in mine:
            pl.when(on)(c.start)
        self.barrier()
        for on, c in mine:
            pl.when(on)(c.wait)
        ks = [2 * i + self.c for i in range(4)]
        self.z_hop(0)
        self.y_own()
        self.z_hop(1)
        self.z_hop(2)
        self.y_forward(None)
        self.z_hop(3)
        self.x_send(None)
        self.z_hop(4)
        self.x_forward(None)
        self.z_hop(5)
        self.z_hop(6)
        self.z_hop(7)
        self.x_sibling()
        for k in ks:
            self.y_forward(k)
        for k in ks:
            self.x_send(k)
        for k in ks:
            self.x_forward(k)
        for k in ks:
            self.finish(k)
        self.finish(None)
        self.from_sibling()
        self.drain()

N_SEND = 640

def comm_scratch():
    D = pltpu.SemaphoreType.DMA
    return [D((N_SEND,)), D((8, 10, 4)), D((8, 4)), D((8,)), D((8, 8)), D((3,))]

from jax.sharding import PartitionSpec as P


def entry(own, out_ref, g, y, own_sem, *rest):
    p, q = lax.axis_index("row"), lax.axis_index("col")
    n = len(comm_scratch())
    mine = pltpu.make_async_copy(own, out_ref, own_sem)
    mine.start()
    Comm(p, q, own, g, y, *rest[:n]).run()
    mine.wait()
    row = jnp.minimum(p, 7)

    def fill(k, _):
        g[k, row] = g[k, 8]
        return 0
    lax.fori_loop(0, jnp.where(p < 8, p + 1, 0), fill, 0)
    compute(p, q, g, y, out_ref, *rest[n:])


def on_device(matrix):
    own = matrix.reshape(2, B, 2 * B)
    out = pl.pallas_call(
        entry,
        out_shape=jax.ShapeDtypeStruct((2, B, 2 * B), F32),
        in_specs=[pl.BlockSpec(memory_space=pl.ANY)],
        out_specs=pl.BlockSpec(memory_space=pltpu.VMEM),
        scratch_shapes=[pltpu.VMEM((STEPS, SLOTS, B, B), F32), pltpu.VMEM((STEPS, B, 2 * B), F32),
                        pltpu.SemaphoreType.DMA] + comm_scratch() + scratch(),
        compiler_params=pltpu.CompilerParams(vmem_limit_bytes=63 * 1024 * 1024, collective_id=0, has_side_effects=True),
        name="steps",
    )(own)
    return out.reshape(matrix.shape)


def solution(mesh):
    spec = P(None, "row", None, None, "col", None)
    return jax.shard_map(on_device, mesh=mesh, in_specs=(spec,), out_specs=spec, check_vma=False)
```

```python
import jax, jax.numpy as jnp, functools
from jax import lax
from jax.experimental import pallas as pl
from jax.experimental.pallas import tpu as pltpu

F32, BF16 = jnp.float32, jnp.bfloat16

def over_lanes(v, c):
    return jnp.broadcast_to(v[:, c:c + 1], (8, 128))

def over_rows(v, r):
    return jnp.broadcast_to(v[r:r + 1, :], (8, 128))

def eliminate(rows):
    sub = lax.broadcasted_iota(jnp.int32, (8, 128), 0)
    rows = list(rows)
    diag = [over_lanes(rows[0], t) for t in range(8)]
    for s in range(8):
        off = {i: [over_lanes(rows[i], 8 * s + m) for m in range(8)] for i in range(s + 1, 8)}
        nxt = [over_lanes(rows[s + 1], 8 * (s + 1) + t) for t in range(8)] if s < 7 else None
        top = rows[s]
        for m in range(8):
            root = lax.rsqrt(over_rows(diag[m], m))
            lead = diag[m] * root
            unit = over_rows(top, m) * root
            top = jnp.where(sub == m, unit, top - jnp.where(sub > m, lead, 0.0) * unit)
            scal = {t: over_rows(lead, t) for t in range(m + 1, 8)}
            for t in range(m + 1, 8):
                diag[t] = diag[t] - lead * scal[t]
            for i in range(s + 1, 8):
                mult = off[i][m] * root
                for t in range(m + 1, 8):
                    off[i][t] = off[i][t] - mult * scal[t]
                rows[i] = rows[i] - mult * unit
                if i == s + 1:
                    for t in range(8):
                        nxt[t] = nxt[t] - mult * over_rows(mult, t)
        rows[s] = top
        diag = nxt
    return rows

def split(x):
    hi = x.astype(BF16)
    return hi, (x - hi.astype(F32)).astype(BF16)

def nt(a, b):
    return lax.dot_general(a, b, (((1,), (1,)), ((), ())), preferred_element_type=F32)

def nn(a, b):
    return lax.dot_general(a, b, (((1,), (0,)), ((), ())), preferred_element_type=F32)

def factor_tile(tb, ud, lb, zpad, w_hi, w_lo, before=None, beside=None):
    low = lax.broadcasted_iota(jnp.int32, (64, 128), 1) < 64
    eye = jnp.where(
        lax.broadcasted_iota(jnp.int32, (64, 128), 1)
        == lax.broadcasted_iota(jnp.int32, (64, 128), 0) + 64, 1.0, 0.0).astype(F32)
    zpad[...] = jnp.zeros_like(zpad)

    def group(g, _):
        if before is not None:
            before(g)
        if beside is not None:
            beside(g)
        block = jnp.where(low, tb[g, g], eye)
        done = eliminate([block[8 * i:8 * i + 8] for i in range(8)])
        m = jnp.concatenate(done, 0)
        ud[g] = m
        wz = jnp.where(low, 0.0, m)
        wz_hi, wz_lo = split(wz)
        tcol = tb[:, g].reshape(256, 128)
        t_hi, t_lo = split(tcol)
        w2_hi = jnp.concatenate([wz_hi, wz_hi], 0)
        w2_lo = jnp.concatenate([wz_lo, wz_lo], 0)
        p = nt(jnp.concatenate([t_hi, t_lo], 1), jnp.concatenate([w2_hi, w2_hi], 1)) + nt(t_hi, w2_lo)
        rowblk = lax.broadcasted_iota(jnp.int32, (256, 128), 0) // 64
        p = jnp.where(rowblk > g, p, 0.0)
        lb[:, g] = p.reshape(4, 64, 128)
        hi = p.astype(BF16)
        hif = hi.astype(F32)
        lof = p - hif
        lo = lof.astype(BF16)
        lowp = lax.broadcasted_iota(jnp.int32, (256, 128), 1) < 64
        lhs = jnp.concatenate([jnp.where(lowp, hif, lof).astype(BF16),
                               jnp.where(lowp, hif, 0.0).astype(BF16)], 1)
        for h in range(2):
            parts = []
            for j in (2 * h, 2 * h + 1):
                pj = jnp.concatenate([hi[64 * j:64 * j + 64], lo[64 * j:64 * j + 64]], 1)
                parts += [pj, pj]
            upd = nt(lhs, jnp.concatenate(parts, 0))
            for j in range(2):
                tb[:, 2 * h + j] = tb[:, 2 * h + j] - upd[:, 128 * j:128 * j + 128].reshape(4, 64, 128)
        z = zpad[pl.ds(pl.multiple_of(64 * g, 64), 128), :]
        z_hi, z_lo = split(z)
        mix = nn(jnp.concatenate([wz_hi, wz_lo], 1), jnp.concatenate([z_hi, z_hi], 0)) + nn(wz_hi, z_lo)
        turned = pltpu.roll(m, 64, 1)
        both = jnp.where(low, turned, m)
        here = lax.broadcasted_iota(jnp.int32, (64, 256), 1) // 64 == g
        wrow = jnp.where(here, jnp.concatenate([both, both], 1), -mix)
        at = pl.ds(pl.multiple_of(64 * g, 64), 64)
        r_hi, r_lo = split(wrow)
        w_hi[at, :] = r_hi
        w_lo[at, :] = r_lo
        zpad[64:, :] = zpad[64:, :] + nn(lhs, jnp.concatenate([r_hi, r_hi, r_lo, r_lo], 0))
        return 0
    lax.fori_loop(0, 4, group, 0)

def blocks(tile, tb):
    low = lax.broadcasted_iota(jnp.int32, (256, 128), 1) < 64
    for h in range(2):
        x = tile[:, 128 * h:128 * h + 128]
        r = pltpu.roll(x, 64, 1)
        tb[:, 2 * h] = jnp.where(low, x, r).reshape(4, 64, 128)
        tb[:, 2 * h + 1] = jnp.where(low, r, x).reshape(4, 64, 128)


B = 256
STEPS = 8
SLOTS = 10

def nt3(ah, al, bh, bl):
    return nt(ah, bh) + nt(ah, bl) + nt(al, bh)

def nn3(ah, al, bh, bl):
    return nn(ah, bh) + nn(ah, bl) + nn(al, bh)

def pair(r):
    return pl.ds(2 * r, 2)

def lead_factor(p, q, g, lh, ll, wh, wl, tb, ud, lb, zpad, held, ready, pump):
    def apply(j, r, m):
        got = nt3(lh[m, pair(r)].reshape(512, B), ll[m, pair(r)].reshape(512, B), lh[m, j], ll[m, j])
        g[j, pair(r)] = g[j, pair(r)] - got.reshape(2, B, B)

    def step(k, _):
        ready(k)

        def last(r, _):
            apply(k, r, k - 1)
            return 0
        lax.fori_loop(jnp.where(k > 0, k // 2, 4), 4, last, 0)
        blocks(g[k, k], tb)

        def beside(i):
            j = k + 1
            rows = jnp.maximum(4 - j // 2, 1)
            for n in range(2):
                turn = 2 * i + n
                m = turn // rows
                on = (m < k) & (j < STEPS)
                apply(jnp.where(on, j, 7), jnp.where(on, j // 2 + turn % rows, 0), jnp.where(on, m, 0))

        factor_tile(tb, ud, lb, zpad, wh.at[k], wl.at[k], lambda i: pump(4 * k + i), beside)

        def solve(r, _):
            ah, al = split(g[k, pair(r)].reshape(512, B))
            got = nt3(ah, al, wh[k], wl[k]).reshape(2, B, B)
            hi, lo = split(got)
            lh[k, pair(r)] = hi
            ll[k, pair(r)] = lo
            return 0
        lax.fori_loop(k // 2, 4, solve, 0)

        @pl.when((q == k) & (p == k))
        def _():
            low = lax.broadcasted_iota(jnp.int32, (64, 128), 1) < 64
            tri = lax.broadcasted_iota(jnp.int32, (64, 128), 0) <= lax.broadcasted_iota(jnp.int32, (64, 128), 1)
            for i in range(4):
                up = jnp.where(tri & low, ud[i], 0.0)
                turned = jnp.concatenate([up, jnp.zeros((64, 128), F32)], 0).T[:64]
                twice = turned + pltpu.roll(turned, 64, 1)
                parts = [lb[i, j] if j < i else (twice if j == i else jnp.zeros((64, 128), F32)) for j in range(4)]
                for h in range(2):
                    held[0, 64 * i:64 * i + 64, 128 * h:128 * h + 128] = jnp.where(low, parts[2 * h], parts[2 * h + 1])
        return 0
    lax.fori_loop(0, STEPS, step, 0)

def own_panels(p, q, g, y, out_ref, lh, ll, wh, wl, held):
    def step(k, _):
        ah, al = split(g[k, 8:10].reshape(512, B))
        left = nt3(ah, al, wh[k], wl[k])
        left = jnp.concatenate([jnp.where(p > k, left[:B], 0.0), left[B:]], 0)
        xh, xl = split(left)
        yh, yl = split(y[k])
        up = nn3(wh[k], wl[k], yh, yl)
        up = jnp.concatenate([jnp.where(q > k, up[:, :B], 0.0), up[:, B:]], 1)
        uh, ul = split(up)
        lh[k, 8:10] = xh.reshape(2, B, B)
        ll[k, 8:10] = xl.reshape(2, B, B)
        y[k] = up

        @pl.when((q == k) & (p != k))
        def _():
            held[0] = left[:B]

        @pl.when(q == k)
        def _():
            held[1] = left[B:]

        for a in range(2):
            out_ref[a] = out_ref[a] - nn3(xh[B * a:B * a + B], xl[B * a:B * a + B], uh, ul)

        def later(j, _):
            xh = lh[k, 8:10].reshape(512, B)
            xl = ll[k, 8:10].reshape(512, B)
            uh, ul = split(y[k])
            g[j, 8:10] = g[j, 8:10] - nt3(xh, xl, lh[k, j], ll[k, j]).reshape(2, B, B)
            y[j] = y[j] - nn3(lh[k, j], ll[k, j], uh, ul)
            return 0
        lax.fori_loop(k + 1, STEPS, later, 0)
        return 0
    lax.fori_loop(0, STEPS, step, 0)

    @pl.when(q < STEPS)
    def _():
        out_ref[:, :, :B] = held[...]

def scratch():
    V = pltpu.VMEM
    return [V((STEPS, SLOTS, B, B), BF16), V((STEPS, SLOTS, B, B), BF16),
            V((STEPS, B, B), BF16), V((STEPS, B, B), BF16),
            V((4, 4, 64, 128), F32), V((4, 64, 128), F32), V((4, 4, 64, 128), F32), V((320, B), F32),
            V((2, B, B), F32)]
MESH = pl.DeviceIdType.MESH

class Comm:
    def __init__(self, p, q, own, g, y, send_sem, g_sem, y_sem, x_sem, d_sem, own_sem):
        self.p, self.q, self.own, self.g, self.y = p, q, own, g, y
        self.px, self.py, self.pz, self.c = p % 4, p // 4, q // 2, q % 2
        self.send_sem, self.g_sem, self.y_sem = send_sem, g_sem, y_sem
        self.x_sem, self.d_sem, self.own_sem = x_sem, d_sem, own_sem
        self.base, self.next, self.waiting = self.layout()[0], 0, False

    def at_z(self, d):
        return (self.p, 2 * ((self.pz + d) % 8) + self.c)

    def at_y(self, d):
        return (4 * ((self.py + d) % 4) + self.px, self.q)

    def at_x(self, d):
        return (4 * self.py + (self.px + d) % 4, self.q)

    def sibling(self):
        return (self.p, 2 * self.pz + 1 - self.c)

    def barrier(self):
        b = pltpu.get_barrier_semaphore()
        peers = [self.at_z(1), self.at_z(-1), self.at_y(1), self.at_y(-1), self.at_x(1), self.at_x(-1), self.sibling()]
        for d in peers:
            pl.semaphore_signal(b, inc=1, device_id=d, device_id_type=MESH)
        pl.semaphore_wait(b, len(peers))

    def send(self, cond, src, dst, sem, to):
        c = pltpu.make_async_remote_copy(src_ref=src, dst_ref=dst, send_sem=self.send_sem.at[self.next],
                                         recv_sem=sem, device_id=to, device_id_type=MESH)
        self.next += 1
        pl.when(cond)(c.wait_send if self.waiting else c.start)

    def take(self, cond, ref, sem):
        if self.waiting:
            return
        c = pltpu.make_async_remote_copy(src_ref=ref, dst_ref=ref, send_sem=self.send_sem.at[0],
                                         recv_sem=sem, device_id=self.sibling(), device_id_type=MESH)
        pl.when(cond)(c.wait_recv)

    @staticmethod
    def count(name, args):
        if name == "z_hop":
            return 4 * (3 if args[1] == 0 else 1)
        if name == "y_own":
            return 8
        if name in ("y_forward", "x_sibling"):
            return 4
        rows = len(args[1]) if len(args) > 1 else 2
        tile = args[0] is not None
        return rows * {"x_send": 8 + tile, "x_forward": 4, "finish": 3 * tile}[name]

    @classmethod
    def layout(cls):
        every = list(cls.BEGIN) + [op for n in sorted(cls.SCHEDULE) for op in cls.SCHEDULE[n]]
        base, at = {}, 0
        for name, *args in every:
            base[name, tuple(args)] = at
            at += cls.count(name, args)
        return base, at

    def do(self, name, *args):
        self.next = self.base[name, args]
        getattr(self, name)(*args)
        assert self.next <= self.base[name, args] + self.count(name, args), (name, args)

    def drain(self, name, *args):
        self.waiting = True
        self.do(name, *args)
        self.waiting = False

    def local(self):
        p, q = self.p, self.q
        lead = jnp.minimum(q, 7)
        rowk = jnp.minimum(p, 7)
        return [(q < 8, pltpu.make_async_copy(self.own.at[a, :, pl.ds(0, B)], self.g.at[lead, 8 + a], self.own_sem.at[a]))
                for a in range(2)] + [
            (p < 8, pltpu.make_async_copy(self.own.at[0], self.y.at[rowk], self.own_sem.at[2]))]

    def gp(self, k, slot, piece):
        return self.g.at[k, slot, pl.ds(64 * piece, 64)]

    def z_hop(self, s, a):
        for d, pieces in ((1, (0, 1)), (-1, (2, 3))):
            zs = (self.pz - d * s) % 8
            on = zs < 4
            k = jnp.minimum(2 * zs + self.c, 7)
            if True:
                for piece in pieces:
                    ref, sem = self.gp(k, 8 + a, piece), self.g_sem.at[k, 8 + a, piece]
                    if s > 0:
                        self.take(on, ref, sem)
                    if s < 7:
                        self.send(on, ref, ref, sem, self.at_z(d))
                    if a == 0:
                        row = on & (self.p < 8) & (k <= self.p)
                        pp = jnp.minimum(self.p, 7)
                        for e in (1, -1):
                            self.send(row, ref, self.gp(k, pp, piece), self.g_sem.at[k, pp, piece], self.at_y(e))

    def y_own(self):
        pp = jnp.minimum(self.p, 7)
        for piece in range(4):
            ref = self.y.at[pp, pl.ds(64 * piece, 64)]
            for e in (1, -1):
                self.send(self.p < 8, ref, ref, self.y_sem.at[pp, piece], self.at_y(e))

    def item(self, i):
        k = None if i is None else 2 * i + self.c
        if k is None:
            ref = lambda r, piece: self.y.at[r, pl.ds(64 * piece, 64)]
            return ref, ref, (lambda r, piece: self.y_sem.at[r, piece]), (lambda r: True)
        return ((lambda r, piece: self.gp(k, jnp.where(r == self.p, 8, r), piece)),
                (lambda r, piece: self.gp(k, r, piece)),
                (lambda r, piece: self.g_sem.at[k, r, piece]),
                (lambda r: k <= r))

    def y_forward(self, k):
        src, dst, sem, has = self.item(k)
        k = None if k is None else 2 * k + self.c
        for d, pieces in ((1, (0, 1)), (-1, (2, 3))):
            ys = (self.py - d) % 4
            r = jnp.minimum(4 * ys + self.px, 7)
            on = (ys < 2) & has(r)
            for piece in pieces:
                self.take(on, dst(r, piece), sem(r, piece))
                self.send(on, dst(r, piece), dst(r, piece), sem(r, piece), self.at_y(d))

    def x_send(self, k, rows=(0, 1)):
        src, dst, sem, has = self.item(k)
        k = None if k is None else 2 * k + self.c
        for ys in rows:
            r = 4 * ys + self.px
            dist = (self.py - ys) % 4
            for piece in range(4):
                rest = (dist == 2) | (dist == (1 if piece >= 2 else 3))
                self.take(rest & has(r), dst(r, piece), sem(r, piece))
                for e in (1, -1):
                    self.send(jnp.bool_(True) & has(r), src(r, piece), dst(r, piece), sem(r, piece), self.at_x(e))
            if k is not None:
                self.send(has(r) & (dist != 0), self.g.at[k, r], self.g.at[k, r], self.d_sem.at[k, r], self.sibling())

    def x_forward(self, k, rows=(0, 1)):
        src, dst, sem, has = self.item(k)
        k = None if k is None else 2 * k + self.c
        for d, pieces in ((1, (0, 1)), (-1, (2, 3))):
            xs = (self.px - d) % 4
            for ys in rows:
                r = 4 * ys + xs
                for piece in pieces:
                    self.take(jnp.bool_(True) & has(r), dst(r, piece), sem(r, piece))
                    self.send(jnp.bool_(True) & has(r), dst(r, piece), dst(r, piece), sem(r, piece), self.at_x(d))

    def finish(self, k, rows=(0, 1)):
        src, dst, sem, has = self.item(k)
        k = None if k is None else 2 * k + self.c
        for dx in (1, 3, 2):
            xs = (self.px - dx) % 4
            pieces = {1: (2, 3), 3: (0, 1), 2: (0, 1, 2, 3)}[dx]
            for ys in rows:
                r = 4 * ys + xs
                for piece in pieces:
                    self.take(jnp.bool_(True) & has(r), dst(r, piece), sem(r, piece))
                if k is not None:
                    self.send(has(r), self.g.at[k, r], self.g.at[k, r], self.d_sem.at[k, r], self.sibling())

    def x_sibling(self, a):
        for i in range(4):
            k = 2 * i + self.c
            self.send(k < 8, self.g.at[k, 8 + a], self.g.at[k, 8 + a], self.x_sem.at[k, a], self.sibling())

    def from_sibling(self, i):
        k = 2 * i + 1 - self.c
        self.take(k < 8, self.g.at[k, 8], self.x_sem.at[k, 0])
        for r in range(8):
            self.take((k <= r) & (r != self.p), self.g.at[k, r], self.d_sem.at[k, r])

    def from_sibling_late(self):
        for i in range(4):
            k = 2 * i + 1 - self.c
            self.take(k < 8, self.g.at[k, 9], self.x_sem.at[k, 1])

    def begin(self):
        mine = self.local()
        for on, c in mine:
            pl.when(on)(c.start)
        self.barrier()
        for on, c in mine:
            pl.when(on)(c.wait)
        for op in self.BEGIN:
            self.do(*op)

    BEGIN = (
        [("z_hop", 0, 0), ("y_own",), ("z_hop", 1, 0), ("z_hop", 2, 0), ("y_forward", None), ("x_send", None, (0,))]
        + [("z_hop", s, 0) for s in range(3, 8)]
        + [("x_sibling", 0), ("z_hop", 0, 1), ("y_forward", 0), ("x_send", 0), ("y_forward", 1), ("x_forward", 0),
           ("finish", 0), ("x_send", 1)]
    )

    SCHEDULE = {
        0: [("x_forward", 1), ("z_hop", 1, 1)],
        1: [("finish", 1), ("y_forward", 2)],
        2: [("x_send", 2), ("z_hop", 2, 1)],
        3: [("x_forward", 2)],
        4: [("finish", 2), ("z_hop", 3, 1)],
        5: [("y_forward", 3), ("x_send", 3)],
        6: [("z_hop", 4, 1)],
        7: [("x_forward", 3)],
        8: [("finish", 3), ("z_hop", 5, 1)],
        9: [("x_send", None, (1,))],
        10: [("z_hop", 6, 1)],
        11: [("x_forward", None, (0,))],
        12: [("z_hop", 7, 1), ("x_sibling", 1)],
        13: [("x_forward", None, (1,))],
        16: [("finish", None)],
    }

    def pump(self, it):
        for top in range(0, 20, 4):
            @pl.when(it // 4 == top // 4)
            def _():
                for n in range(top, top + 4):
                    if n in self.SCHEDULE:
                        @pl.when(it == n)
                        def _():
                            for op in self.SCHEDULE[n]:
                                self.do(*op)

    def ready(self, k):
        for i in range(4):
            @pl.when(k == max(2 * i - 1, 0))
            def _():
                self.from_sibling(i)
                for name in ("y_forward", "x_send", "x_forward", "finish"):
                    self.drain(name, i)
                row = jnp.minimum(self.p, 7)
                for col in (2 * i, 2 * i + 1):
                    @pl.when((self.p < 8) & (col <= self.p))
                    def _():
                        self.g[col, row] = self.g[col, 8]

    def end(self):
        self.from_sibling_late()
        done = {(n, (i,)) for n in ("y_forward", "x_send", "x_forward", "finish") for i in range(4)}
        for name, args in list(self.base):
            if (name, args) not in done:
                self.drain(name, *args)


def comm_scratch():
    D = pltpu.SemaphoreType.DMA
    return [D((Comm.layout()[1],)), D((8, 10, 4)), D((8, 4)), D((8, 2)), D((8, 8)), D((3,))]

from jax.sharding import PartitionSpec as P


def entry(own, out_ref, g, y, own_sem, *rest):
    p, q = lax.axis_index("row"), lax.axis_index("col")
    n = len(comm_scratch())
    lh, ll, wh, wl, *work, held = rest[n:]
    mine = pltpu.make_async_copy(own, out_ref, own_sem)
    mine.start()
    comm = Comm(p, q, own, g, y, *rest[:n])
    comm.begin()
    lead_factor(p, q, g, lh, ll, wh, wl, *work, held, comm.ready, comm.pump)
    mine.wait()
    comm.end()
    own_panels(p, q, g, y, out_ref, lh, ll, wh, wl, held)


def on_device(matrix):
    own = matrix.reshape(2, B, 2 * B)
    out = pl.pallas_call(
        entry,
        out_shape=jax.ShapeDtypeStruct((2, B, 2 * B), F32),
        in_specs=[pl.BlockSpec(memory_space=pl.ANY)],
        out_specs=pl.BlockSpec(memory_space=pltpu.VMEM),
        scratch_shapes=[pltpu.VMEM((STEPS, SLOTS, B, B), F32), pltpu.VMEM((STEPS, B, 2 * B), F32),
                        pltpu.SemaphoreType.DMA] + comm_scratch() + scratch(),
        compiler_params=pltpu.CompilerParams(vmem_limit_bytes=63 * 1024 * 1024, collective_id=0, has_side_effects=True),
        name="steps",
    )(own)
    return out.reshape(matrix.shape)


def solution(mesh):
    spec = P(None, "row", None, None, "col", None)
    return jax.shard_map(on_device, mesh=mesh, in_specs=(spec,), out_specs=spec, check_vma=False)
```

```python
import jax, jax.numpy as jnp, functools
from jax import lax
from jax.experimental import pallas as pl
from jax.experimental.pallas import tpu as pltpu

F32, BF16 = jnp.float32, jnp.bfloat16

def over_lanes(v, c):
    return jnp.broadcast_to(v[:, c:c + 1], (8, 128))

def over_rows(v, r):
    return jnp.broadcast_to(v[r:r + 1, :], (8, 128))

def eliminate(rows):
    sub = lax.broadcasted_iota(jnp.int32, (8, 128), 0)
    rows = list(rows)
    diag = [over_lanes(rows[0], t) for t in range(8)]
    for s in range(8):
        off = {i: [over_lanes(rows[i], 8 * s + m) for m in range(8)] for i in range(s + 1, 8)}
        nxt = [over_lanes(rows[s + 1], 8 * (s + 1) + t) for t in range(8)] if s < 7 else None
        top = rows[s]
        for m in range(8):
            root = lax.rsqrt(over_rows(diag[m], m))
            lead = diag[m] * root
            unit = over_rows(top, m) * root
            top = jnp.where(sub == m, unit, top - jnp.where(sub > m, lead, 0.0) * unit)
            scal = {t: over_rows(lead, t) for t in range(m + 1, 8)}
            for t in range(m + 1, 8):
                diag[t] = diag[t] - lead * scal[t]
            for i in range(s + 1, 8):
                mult = off[i][m] * root
                for t in range(m + 1, 8):
                    off[i][t] = off[i][t] - mult * scal[t]
                rows[i] = rows[i] - mult * unit
                if i == s + 1:
                    for t in range(8):
                        nxt[t] = nxt[t] - mult * over_rows(mult, t)
        rows[s] = top
        diag = nxt
    return rows

def split(x):
    hi = x.astype(BF16)
    return hi, (x - hi.astype(F32)).astype(BF16)

def nt(a, b):
    return lax.dot_general(a, b, (((1,), (1,)), ((), ())), preferred_element_type=F32)

def nn(a, b):
    return lax.dot_general(a, b, (((1,), (0,)), ((), ())), preferred_element_type=F32)

def factor_tile(tb, ud, lb, zpad, w_hi, w_lo, before=None, beside=None):
    low = lax.broadcasted_iota(jnp.int32, (64, 128), 1) < 64
    eye = jnp.where(
        lax.broadcasted_iota(jnp.int32, (64, 128), 1)
        == lax.broadcasted_iota(jnp.int32, (64, 128), 0) + 64, 1.0, 0.0).astype(F32)
    zpad[...] = jnp.zeros_like(zpad)

    def group(g, _):
        if before is not None:
            before(g)
        if beside is not None:
            beside(g)
        block = jnp.where(low, tb[g, g], eye)
        done = eliminate([block[8 * i:8 * i + 8] for i in range(8)])
        m = jnp.concatenate(done, 0)
        ud[g] = m
        wz = jnp.where(low, 0.0, m)
        wz_hi, wz_lo = split(wz)
        tcol = tb[:, g].reshape(256, 128)
        t_hi, t_lo = split(tcol)
        w2_hi = jnp.concatenate([wz_hi, wz_hi], 0)
        w2_lo = jnp.concatenate([wz_lo, wz_lo], 0)
        p = nt(jnp.concatenate([t_hi, t_lo], 1), jnp.concatenate([w2_hi, w2_hi], 1)) + nt(t_hi, w2_lo)
        rowblk = lax.broadcasted_iota(jnp.int32, (256, 128), 0) // 64
        p = jnp.where(rowblk > g, p, 0.0)
        lb[:, g] = p.reshape(4, 64, 128)
        hi = p.astype(BF16)
        hif = hi.astype(F32)
        lof = p - hif
        lo = lof.astype(BF16)
        lowp = lax.broadcasted_iota(jnp.int32, (256, 128), 1) < 64
        lhs = jnp.concatenate([jnp.where(lowp, hif, lof).astype(BF16),
                               jnp.where(lowp, hif, 0.0).astype(BF16)], 1)
        for h in range(2):
            parts = []
            for j in (2 * h, 2 * h + 1):
                pj = jnp.concatenate([hi[64 * j:64 * j + 64], lo[64 * j:64 * j + 64]], 1)
                parts += [pj, pj]
            upd = nt(lhs, jnp.concatenate(parts, 0))
            for j in range(2):
                tb[:, 2 * h + j] = tb[:, 2 * h + j] - upd[:, 128 * j:128 * j + 128].reshape(4, 64, 128)
        z = zpad[pl.ds(pl.multiple_of(64 * g, 64), 128), :]
        z_hi, z_lo = split(z)
        mix = nn(jnp.concatenate([wz_hi, wz_lo], 1), jnp.concatenate([z_hi, z_hi], 0)) + nn(wz_hi, z_lo)
        turned = pltpu.roll(m, 64, 1)
        both = jnp.where(low, turned, m)
        here = lax.broadcasted_iota(jnp.int32, (64, 256), 1) // 64 == g
        wrow = jnp.where(here, jnp.concatenate([both, both], 1), -mix)
        at = pl.ds(pl.multiple_of(64 * g, 64), 64)
        r_hi, r_lo = split(wrow)
        w_hi[at, :] = r_hi
        w_lo[at, :] = r_lo
        zpad[64:, :] = zpad[64:, :] + nn(lhs, jnp.concatenate([r_hi, r_hi, r_lo, r_lo], 0))
        return 0
    lax.fori_loop(0, 4, group, 0)

def blocks(tile, tb):
    low = lax.broadcasted_iota(jnp.int32, (256, 128), 1) < 64
    for h in range(2):
        x = tile[:, 128 * h:128 * h + 128]
        r = pltpu.roll(x, 64, 1)
        tb[:, 2 * h] = jnp.where(low, x, r).reshape(4, 64, 128)
        tb[:, 2 * h + 1] = jnp.where(low, r, x).reshape(4, 64, 128)


B = 256
STEPS = 8
SLOTS = 10

def nt3(ah, al, bh, bl):
    return nt(ah, bh) + nt(ah, bl) + nt(al, bh)

def nn3(ah, al, bh, bl):
    return nn(ah, bh) + nn(ah, bl) + nn(al, bh)

def pair(r):
    return pl.ds(2 * r, 2)

def lead_factor(p, q, g, lh, ll, wh, wl, tb, ud, lb, zpad, held, ready, ready_rest, pump):
    def apply(j, r, m):
        got = nt3(lh[m, pair(r)].reshape(512, B), ll[m, pair(r)].reshape(512, B), lh[m, j], ll[m, j])
        g[j, pair(r)] = g[j, pair(r)] - got.reshape(2, B, B)

    def step(k, _):
        ready(k)

        def last(r, _):
            def term(m, _):
                apply(k, r, m)
                return 0
            return lax.fori_loop(jnp.where(k == 2, 0, k - 1), k, term, 0)
        lax.fori_loop(jnp.where(k > 0, k // 2, 4), 4, last, 0)
        blocks(g[k, k], tb)

        def beside(i):
            j = k + 1
            rows = jnp.maximum(4 - j // 2, 1)
            for n in range(2):
                turn = 2 * i + n
                m = turn // rows
                on = (m < k) & (j < STEPS) & (j != 2)
                apply(jnp.where(on, j, 7), jnp.where(on, j // 2 + turn % rows, 0), jnp.where(on, m, 0))

        factor_tile(tb, ud, lb, zpad, wh.at[k], wl.at[k], lambda i: pump(4 * k + i), beside)
        ready_rest(k)

        def solve(r, _):
            ah, al = split(g[k, pair(r)].reshape(512, B))
            got = nt3(ah, al, wh[k], wl[k]).reshape(2, B, B)
            hi, lo = split(got)
            lh[k, pair(r)] = hi
            ll[k, pair(r)] = lo
            return 0
        lax.fori_loop(k // 2, 4, solve, 0)

        @pl.when((q == k) & (p == k))
        def _():
            low = lax.broadcasted_iota(jnp.int32, (64, 128), 1) < 64
            tri = lax.broadcasted_iota(jnp.int32, (64, 128), 0) <= lax.broadcasted_iota(jnp.int32, (64, 128), 1)
            for i in range(4):
                up = jnp.where(tri & low, ud[i], 0.0)
                turned = jnp.concatenate([up, jnp.zeros((64, 128), F32)], 0).T[:64]
                twice = turned + pltpu.roll(turned, 64, 1)
                parts = [lb[i, j] if j < i else (twice if j == i else jnp.zeros((64, 128), F32)) for j in range(4)]
                for h in range(2):
                    held[0, 64 * i:64 * i + 64, 128 * h:128 * h + 128] = jnp.where(low, parts[2 * h], parts[2 * h + 1])
        return 0
    lax.fori_loop(0, STEPS, step, 0)

def own_panels(p, q, g, y, tiles, out_ref, lh, ll, wh, wl, held):
    def step(k, _):
        ah, al = split(g[k, 8:10].reshape(512, B))
        left = nt3(ah, al, wh[k], wl[k])
        left = jnp.concatenate([jnp.where(p > k, left[:B], 0.0), left[B:]], 0)
        xh, xl = split(left)
        yh, yl = split(y[k])
        up = nn3(wh[k], wl[k], yh, yl)
        up = jnp.concatenate([jnp.where(q > k, up[:, :B], 0.0), up[:, B:]], 1)
        uh, ul = split(up)
        lh[k, 8:10] = xh.reshape(2, B, B)
        ll[k, 8:10] = xl.reshape(2, B, B)
        y[k] = up

        @pl.when((q == k) & (p != k))
        def _():
            held[0] = left[:B]

        @pl.when(q == k)
        def _():
            held[1] = left[B:]

        for a in range(2):
            tiles[a] = tiles[a] - nn3(xh[B * a:B * a + B], xl[B * a:B * a + B], uh, ul)

        def later(j, _):
            xh = lh[k, 8:10].reshape(512, B)
            xl = ll[k, 8:10].reshape(512, B)
            uh, ul = split(y[k])
            g[j, 8:10] = g[j, 8:10] - nt3(xh, xl, lh[k, j], ll[k, j]).reshape(2, B, B)
            y[j] = y[j] - nn3(lh[k, j], ll[k, j], uh, ul)
            return 0
        lax.fori_loop(k + 1, STEPS, later, 0)
        return 0
    lax.fori_loop(0, STEPS, step, 0)

    @pl.when(q < STEPS)
    def _():
        tiles[:, :, :B] = held[...]
    for a in range(2):
        for j in range(4):
            out_ref[pl.ds(4 * B * a + j, B, stride=4), :] = tiles[a, :, 128 * j:128 * j + 128]

def scratch():
    V = pltpu.VMEM
    return [V((STEPS, SLOTS, B, B), BF16), V((STEPS, SLOTS, B, B), BF16),
            V((STEPS, B, B), BF16), V((STEPS, B, B), BF16),
            V((4, 4, 64, 128), F32), V((4, 64, 128), F32), V((4, 4, 64, 128), F32), V((320, B), F32),
            V((2, B, B), F32)]
MESH = pl.DeviceIdType.MESH

class Comm:
    def __init__(self, p, q, own, g, y, send_sem, g_sem, y_sem, x_sem, d_sem):
        self.p, self.q, self.own, self.g, self.y = p, q, own, g, y
        self.px, self.py, self.pz, self.c = p % 4, p // 4, q // 2, q % 2
        self.send_sem, self.g_sem, self.y_sem = send_sem, g_sem, y_sem
        self.x_sem, self.d_sem = x_sem, d_sem
        self.base, self.next, self.waiting = self.layout()[0], 0, False

    def at_z(self, d):
        return (self.p, 2 * ((self.pz + d) % 8) + self.c)

    def at_y(self, d):
        return (4 * ((self.py + d) % 4) + self.px, self.q)

    def at_x(self, d):
        return (4 * self.py + (self.px + d) % 4, self.q)

    def sibling(self):
        return (self.p, 2 * self.pz + 1 - self.c)

    def barrier(self):
        b = pltpu.get_barrier_semaphore()
        peers = [self.at_z(1), self.at_z(-1), self.at_y(1), self.at_y(-1), self.at_x(1), self.at_x(-1), self.sibling()]
        for d in peers:
            pl.semaphore_signal(b, inc=1, device_id=d, device_id_type=MESH)
        pl.semaphore_wait(b, len(peers))

    def send(self, cond, src, dst, sem, to):
        c = pltpu.make_async_remote_copy(src_ref=src, dst_ref=dst, send_sem=self.send_sem.at[self.next],
                                         recv_sem=sem, device_id=to, device_id_type=MESH)
        self.next += 1
        pl.when(cond)(c.wait_send if self.waiting else c.start)

    def take(self, cond, ref, sem):
        if self.waiting:
            return
        c = pltpu.make_async_remote_copy(src_ref=ref, dst_ref=ref, send_sem=self.send_sem.at[0],
                                         recv_sem=sem, device_id=self.sibling(), device_id_type=MESH)
        pl.when(cond)(c.wait_recv)

    @staticmethod
    def count(name, args):
        if name == "z_from":
            return 16 if args[1] == 0 else 8
        if name == "x_sibling":
            return 1
        if name == "y_own":
            return 8
        if name == "y_forward":
            return 4
        rows = len(args[1]) if len(args) > 1 else 2
        tile = args[0] is not None
        return rows * {"x_send": 8 + tile, "x_forward": 4, "finish": 3 * tile}[name]

    @classmethod
    def layout(cls):
        every = list(cls.BEGIN) + [op for n in sorted(cls.SCHEDULE) for op in cls.SCHEDULE[n]]
        base, at = {}, 0
        for name, *args in every:
            base[name, tuple(args)] = at
            at += cls.count(name, args)
        return base, at

    def do(self, name, *args):
        self.next = self.base[name, args]
        getattr(self, name)(*args)
        assert self.next <= self.base[name, args] + self.count(name, args), (name, args)

    def drain(self, name, *args):
        self.waiting = True
        self.do(name, *args)
        self.waiting = False

    def local(self, tiles):
        def half(a, j):
            return self.own[pl.ds(4 * B * a + j, B, stride=4), :]

        for a in range(2):
            for j in range(4):
                tiles[a, :, 128 * j:128 * j + 128] = half(a, j)

        @pl.when(self.q < 8)
        def _():
            k = jnp.minimum(self.q, 7)
            for a in range(2):
                for j in range(2):
                    self.g[k, 8 + a, :, 128 * j:128 * j + 128] = half(a, j)

        @pl.when(self.p < 8)
        def _():
            r = jnp.minimum(self.p, 7)
            for j in range(4):
                self.y[r, :, 128 * j:128 * j + 128] = half(0, j)

    def gp(self, k, slot, piece):
        return self.g.at[k, slot, pl.ds(64 * piece, 64)]

    def z_from(self, zs, a):
        dist = (self.pz - zs) % 8
        k = 2 * zs + self.c
        for piece in range(4):
            ref, sem = self.gp(k, 8 + a, piece), self.g_sem.at[k, 8 + a, piece]
            self.take(dist != 0, ref, sem)
            self.send(dist < 4, ref, ref, sem, self.at_z(1))
            self.send((dist == 0) | (dist > 5), ref, ref, sem, self.at_z(-1))
            if a == 0:
                row = (self.p < 8) & (k <= self.p)
                pp = jnp.minimum(self.p, 7)
                for e in (1, -1):
                    self.send(row, ref, self.gp(k, pp, piece), self.g_sem.at[k, pp, piece], self.at_y(e))

    def x_sibling(self, zs, a):
        k = 2 * zs + self.c
        self.send(k < 8, self.g.at[k, 8 + a], self.g.at[k, 8 + a], self.x_sem.at[k, a], self.sibling())

    def y_own(self):
        pp = jnp.minimum(self.p, 7)
        for piece in range(4):
            ref = self.y.at[pp, pl.ds(64 * piece, 64)]
            for e in (1, -1):
                self.send(self.p < 8, ref, ref, self.y_sem.at[pp, piece], self.at_y(e))

    def item(self, i):
        k = None if i is None else 2 * i + self.c
        if k is None:
            ref = lambda r, piece: self.y.at[r, pl.ds(64 * piece, 64)]
            return ref, ref, (lambda r, piece: self.y_sem.at[r, piece]), (lambda r: True)
        return ((lambda r, piece: self.gp(k, jnp.where(r == self.p, 8, r), piece)),
                (lambda r, piece: self.gp(k, r, piece)),
                (lambda r, piece: self.g_sem.at[k, r, piece]),
                (lambda r: k <= r))

    def y_forward(self, k):
        src, dst, sem, has = self.item(k)
        k = None if k is None else 2 * k + self.c
        for d, pieces in ((1, (0, 1)), (-1, (2, 3))):
            ys = (self.py - d) % 4
            r = jnp.minimum(4 * ys + self.px, 7)
            on = (ys < 2) & has(r)
            for piece in pieces:
                self.take(on, dst(r, piece), sem(r, piece))
                self.send(on, dst(r, piece), dst(r, piece), sem(r, piece), self.at_y(d))

    def x_send(self, k, rows=(0, 1)):
        src, dst, sem, has = self.item(k)
        k = None if k is None else 2 * k + self.c
        for ys in rows:
            r = 4 * ys + self.px
            dist = (self.py - ys) % 4
            for piece in range(4):
                rest = (dist == 2) | (dist == (1 if piece >= 2 else 3))
                self.take(rest & has(r), dst(r, piece), sem(r, piece))
                for e in (1, -1):
                    self.send(jnp.bool_(True) & has(r), src(r, piece), dst(r, piece), sem(r, piece), self.at_x(e))
            if k is not None:
                self.send(has(r) & (dist != 0), self.g.at[k, r], self.g.at[k, r], self.d_sem.at[k, r], self.sibling())

    def x_forward(self, k, rows=(0, 1)):
        src, dst, sem, has = self.item(k)
        k = None if k is None else 2 * k + self.c
        for d, pieces in ((1, (0, 1)), (-1, (2, 3))):
            xs = (self.px - d) % 4
            for ys in rows:
                r = 4 * ys + xs
                for piece in pieces:
                    self.take(jnp.bool_(True) & has(r), dst(r, piece), sem(r, piece))
                    self.send(jnp.bool_(True) & has(r), dst(r, piece), dst(r, piece), sem(r, piece), self.at_x(d))

    def finish(self, k, rows=(0, 1)):
        src, dst, sem, has = self.item(k)
        k = None if k is None else 2 * k + self.c
        for dx in (1, 3, 2):
            xs = (self.px - dx) % 4
            pieces = {1: (2, 3), 3: (0, 1), 2: (0, 1, 2, 3)}[dx]
            for ys in rows:
                r = 4 * ys + xs
                for piece in pieces:
                    self.take(jnp.bool_(True) & has(r), dst(r, piece), sem(r, piece))
                if k is not None:
                    self.send(has(r), self.g.at[k, r], self.g.at[k, r], self.d_sem.at[k, r], self.sibling())

    def from_sibling(self, i, rows):
        k = 2 * i + 1 - self.c
        if 0 in rows:
            self.take(k < 8, self.g.at[k, 8], self.x_sem.at[k, 0])
        for r in rows:
            self.take((k <= r) & (r != self.p), self.g.at[k, r], self.d_sem.at[k, r])

    def from_sibling_late(self):
        for i in range(4):
            k = 2 * i + 1 - self.c
            self.take(k < 8, self.g.at[k, 9], self.x_sem.at[k, 1])

    BEGIN = [("z_from", 0, 0), ("x_sibling", 0, 0), ("y_forward", 0), ("z_from", 1, 0), ("x_send", 0, (0,)),
             ("x_forward", 0, (0,)), ("x_send", 0, (1,)), ("finish", 0, (0,))]

    SCHEDULE = {
        0: [("x_forward", 0, (1,)), ("x_sibling", 1, 0)],
        1: [("finish", 0, (1,)), ("y_forward", 1)],
        2: [("x_send", 1, (0, 1)), ("z_from", 2, 0)],
        3: [("x_forward", 1, (0, 1)), ("x_sibling", 2, 0)],
        4: [("finish", 1, (0, 1)), ("y_forward", 2)],
        5: [("x_send", 2, (0, 1)), ("z_from", 3, 0)],
        6: [("x_forward", 2, (0, 1)), ("x_sibling", 3, 0)],
        7: [("finish", 2, (0, 1))],
        8: [("y_forward", 3), ("z_from", 0, 1)],
        9: [("x_send", 3, (0, 1)), ("y_own",)],
        10: [("x_forward", 3, (0, 1)), ("z_from", 1, 1)],
        11: [("finish", 3, (0, 1)), ("y_forward", None)],
        12: [("x_send", None, (0,)), ("z_from", 2, 1)],
        14: [("x_forward", None, (0,)), ("z_from", 3, 1)],
        15: [("x_send", None, (1,))],
        17: [("x_forward", None, (1,)), ("x_sibling", 0, 1), ("x_sibling", 1, 1), ("x_sibling", 2, 1), ("x_sibling", 3, 1)],
        20: [("finish", None, (0, 1))],
    }

    def begin(self, tiles):
        self.local(tiles)
        self.barrier()
        for op in self.BEGIN:
            self.do(*op)

    def pump(self, it):
        for top in range(0, 24, 4):
            @pl.when(it // 4 == top // 4)
            def _():
                for n in range(top, top + 4):
                    if n in self.SCHEDULE:
                        @pl.when(it == n)
                        def _():
                            for op in self.SCHEDULE[n]:
                                self.do(*op)

    def plane_ops(self, i):
        return [op for op in self.base if op[0] in ("y_forward", "x_send", "x_forward", "finish") and op[1][0] == i]

    def fill(self, i):
        row = jnp.minimum(self.p, 7)
        for col in (2 * i, 2 * i + 1):
            @pl.when((self.p < 8) & (col <= self.p))
            def _():
                self.g[col, row] = self.g[col, 8]

    def ready(self, k):
        @pl.when(k == 0)
        def _():
            self.from_sibling(0, range(4))
            self.fill(0)

        @pl.when(k == 1)
        def _():
            for name, args in self.plane_ops(0):
                self.drain(name, *args)

        for i, at in ((1, 2), (2, 3), (3, 5)):
            @pl.when(k == at)
            def _():
                self.from_sibling(i, range(8))
                self.fill(i)
                for name, args in self.plane_ops(i):
                    self.drain(name, *args)

    def ready_rest(self, k):
        @pl.when(k == 0)
        def _():
            self.from_sibling(0, range(4, 8))

    def end(self):
        self.from_sibling_late()
        done = [op for i in range(4) for op in self.plane_ops(i)]
        for name, args in self.base:
            if (name, args) not in done:
                self.drain(name, *args)

def comm_scratch():
    D = pltpu.SemaphoreType.DMA
    return [D((Comm.layout()[1],)), D((8, 10, 4)), D((8, 4)), D((8, 2)), D((8, 8))]

from jax.sharding import PartitionSpec as P


def entry(own, out_ref, g, y, tiles, *rest):
    p, q = lax.axis_index("row"), lax.axis_index("col")
    n = len(comm_scratch())
    lh, ll, wh, wl, *work, held = rest[n:]
    comm = Comm(p, q, own, g, y, *rest[:n])
    comm.begin(tiles)
    lead_factor(p, q, g, lh, ll, wh, wl, *work, held, comm.ready, comm.ready_rest, comm.pump)
    comm.end()
    own_panels(p, q, g, y, tiles, out_ref, lh, ll, wh, wl, held)


def on_device(matrix):
    out = pl.pallas_call(
        entry,
        out_shape=jax.ShapeDtypeStruct((8 * B, 128), F32),
        in_specs=[pl.BlockSpec(memory_space=pltpu.VMEM)],
        out_specs=pl.BlockSpec(memory_space=pltpu.VMEM),
        scratch_shapes=[pltpu.VMEM((STEPS, SLOTS, B, B), F32), pltpu.VMEM((STEPS, B, 2 * B), F32),
                        pltpu.VMEM((2, B, 2 * B), F32)] + comm_scratch() + scratch(),
        compiler_params=pltpu.CompilerParams(vmem_limit_bytes=63 * 1024 * 1024, collective_id=0, has_side_effects=True),
        name="steps",
    )(matrix.reshape(8 * B, 128))
    return out.reshape(matrix.shape)


def solution(mesh):
    spec = P(None, "row", None, None, "col", None)
    return jax.shard_map(on_device, mesh=mesh, in_specs=(spec,), out_specs=spec, check_vma=False)
```

```python
import jax, jax.numpy as jnp, functools
from jax import lax
from jax.experimental import pallas as pl
from jax.experimental.pallas import tpu as pltpu

F32, BF16 = jnp.float32, jnp.bfloat16

def over_lanes(v, c):
    return jnp.broadcast_to(v[:, c:c + 1], (8, 128))

def over_rows(v, r):
    return jnp.broadcast_to(v[r:r + 1, :], (8, 128))

def eliminate(rows):
    sub = lax.broadcasted_iota(jnp.int32, (8, 128), 0)
    rows = list(rows)
    diag = [over_lanes(rows[0], t) for t in range(8)]
    for s in range(8):
        off = {i: [over_lanes(rows[i], 8 * s + m) for m in range(8)] for i in range(s + 1, 8)}
        nxt = [over_lanes(rows[s + 1], 8 * (s + 1) + t) for t in range(8)] if s < 7 else None
        top = rows[s]
        for m in range(8):
            root = lax.rsqrt(over_rows(diag[m], m))
            lead = diag[m] * root
            unit = over_rows(top, m) * root
            top = jnp.where(sub == m, unit, top - jnp.where(sub > m, lead, 0.0) * unit)
            scal = {t: over_rows(lead, t) for t in range(m + 1, 8)}
            for t in range(m + 1, 8):
                diag[t] = diag[t] - lead * scal[t]
            for i in range(s + 1, 8):
                mult = off[i][m] * root
                for t in range(m + 1, 8):
                    off[i][t] = off[i][t] - mult * scal[t]
                rows[i] = rows[i] - mult * unit
                if i == s + 1:
                    for t in range(8):
                        nxt[t] = nxt[t] - mult * over_rows(mult, t)
        rows[s] = top
        diag = nxt
    return rows

def split(x):
    hi = x.astype(BF16)
    return hi, (x - hi.astype(F32)).astype(BF16)

def nt(a, b):
    return lax.dot_general(a, b, (((1,), (1,)), ((), ())), preferred_element_type=F32)

def nn(a, b):
    return lax.dot_general(a, b, (((1,), (0,)), ((), ())), preferred_element_type=F32)

def factor_tile(tb, ud, lb, zpad, w_hi, w_lo, before=None, beside=None):
    low = lax.broadcasted_iota(jnp.int32, (64, 128), 1) < 64
    eye = jnp.where(
        lax.broadcasted_iota(jnp.int32, (64, 128), 1)
        == lax.broadcasted_iota(jnp.int32, (64, 128), 0) + 64, 1.0, 0.0).astype(F32)
    zpad[...] = jnp.zeros_like(zpad)

    def group(g, _):
        if before is not None:
            before(g)
        if beside is not None:
            beside(g)
        block = jnp.where(low, tb[g, g], eye)
        done = eliminate([block[8 * i:8 * i + 8] for i in range(8)])
        m = jnp.concatenate(done, 0)
        ud[g] = m
        wz = jnp.where(low, 0.0, m)
        wz_hi, wz_lo = split(wz)
        tcol = tb[:, g].reshape(256, 128)
        t_hi, t_lo = split(tcol)
        w2_hi = jnp.concatenate([wz_hi, wz_hi], 0)
        w2_lo = jnp.concatenate([wz_lo, wz_lo], 0)
        p = nt(jnp.concatenate([t_hi, t_lo], 1), jnp.concatenate([w2_hi, w2_hi], 1)) + nt(t_hi, w2_lo)
        rowblk = lax.broadcasted_iota(jnp.int32, (256, 128), 0) // 64
        p = jnp.where(rowblk > g, p, 0.0)
        lb[:, g] = p.reshape(4, 64, 128)
        hi = p.astype(BF16)
        hif = hi.astype(F32)
        lof = p - hif
        lo = lof.astype(BF16)
        lowp = lax.broadcasted_iota(jnp.int32, (256, 128), 1) < 64
        lhs = jnp.concatenate([jnp.where(lowp, hif, lof).astype(BF16),
                               jnp.where(lowp, hif, 0.0).astype(BF16)], 1)
        for h in range(2):
            parts = []
            for j in (2 * h, 2 * h + 1):
                pj = jnp.concatenate([hi[64 * j:64 * j + 64], lo[64 * j:64 * j + 64]], 1)
                parts += [pj, pj]
            upd = nt(lhs, jnp.concatenate(parts, 0))
            for j in range(2):
                tb[:, 2 * h + j] = tb[:, 2 * h + j] - upd[:, 128 * j:128 * j + 128].reshape(4, 64, 128)
        z = zpad[pl.ds(pl.multiple_of(64 * g, 64), 128), :]
        z_hi, z_lo = split(z)
        mix = nn(jnp.concatenate([wz_hi, wz_lo], 1), jnp.concatenate([z_hi, z_hi], 0)) + nn(wz_hi, z_lo)
        turned = pltpu.roll(m, 64, 1)
        both = jnp.where(low, turned, m)
        here = lax.broadcasted_iota(jnp.int32, (64, 256), 1) // 64 == g
        wrow = jnp.where(here, jnp.concatenate([both, both], 1), -mix)
        at = pl.ds(pl.multiple_of(64 * g, 64), 64)
        r_hi, r_lo = split(wrow)
        w_hi[at, :] = r_hi
        w_lo[at, :] = r_lo
        zpad[64:, :] = zpad[64:, :] + nn(lhs, jnp.concatenate([r_hi, r_hi, r_lo, r_lo], 0))
        return 0
    lax.fori_loop(0, 4, group, 0)

def blocks(tile, tb):
    low = lax.broadcasted_iota(jnp.int32, (256, 128), 1) < 64
    for h in range(2):
        x = tile[:, 128 * h:128 * h + 128]
        r = pltpu.roll(x, 64, 1)
        tb[:, 2 * h] = jnp.where(low, x, r).reshape(4, 64, 128)
        tb[:, 2 * h + 1] = jnp.where(low, r, x).reshape(4, 64, 128)


B = 256
STEPS = 8
SLOTS = 10

def nt3(ah, al, bh, bl):
    return nt(ah, bh) + nt(ah, bl) + nt(al, bh)

def nn3(ah, al, bh, bl):
    return nn(ah, bh) + nn(ah, bl) + nn(al, bh)

def pair(r):
    return pl.ds(2 * r, 2)

def lead_factor(p, g, lx, lh, ll, wh, wl, tb, ud, lb, zpad, ready, ready_rest, pump):
    def apply(j, r, m):
        got = nt3(lh[m, pair(r)].reshape(512, B), ll[m, pair(r)].reshape(512, B), lh[m, j], ll[m, j])
        g[j, pair(r)] = g[j, pair(r)] - got.reshape(2, B, B)

    def step(k, _):
        ready(k)

        def last(r, _):
            def term(m, _):
                apply(k, r, m)
                return 0
            return lax.fori_loop(jnp.where(k == 2, 0, k - 1), k, term, 0)
        lax.fori_loop(jnp.where(k > 0, k // 2, 5), 5, last, 0)
        blocks(g[k, k], tb)

        def beside(i):
            j = k + 1
            rows = jnp.maximum(5 - j // 2, 1)
            for n in range(3):
                turn = 3 * i + n
                m = turn // rows
                on = (m < k) & (j < STEPS) & (j != 2)
                apply(jnp.where(on, j, 7), jnp.where(on, j // 2 + turn % rows, 0), jnp.where(on, m, 0))

        factor_tile(tb, ud, lb, zpad, wh, wl, lambda i: pump(k, i), beside)
        ready_rest(k)

        def solve(r):
            ah, al = split(g[k, pair(r)].reshape(512, B))
            return nt3(ah, al, wh[...], wl[...])

        def keep(r, got):
            hi, lo = split(got.reshape(2, B, B))
            lh[k, pair(r)] = hi
            ll[k, pair(r)] = lo

        got = solve(4)
        got = jnp.concatenate([jnp.where(p > k, got[:B], 0.0), got[B:]], 0)
        keep(4, got)
        lx[k] = got.reshape(2, B, B)

        @pl.when(p == k)
        def _():
            low = lax.broadcasted_iota(jnp.int32, (64, 128), 1) < 64
            tri = lax.broadcasted_iota(jnp.int32, (64, 128), 0) <= lax.broadcasted_iota(jnp.int32, (64, 128), 1)
            for i in range(4):
                up = jnp.where(tri & low, ud[i], 0.0)
                turned = jnp.concatenate([up, jnp.zeros((64, 128), F32)], 0).T[:64]
                twice = turned + pltpu.roll(turned, 64, 1)
                parts = [lb[i, j] if j < i else (twice if j == i else jnp.zeros((64, 128), F32)) for j in range(4)]
                for h in range(2):
                    lx[k, 0, 64 * i:64 * i + 64, 128 * h:128 * h + 128] = jnp.where(low, parts[2 * h], parts[2 * h + 1])

        def rest(r, _):
            keep(r, solve(r))
            return 0
        lax.fori_loop(k // 2, 4, rest, 0)
        return 0
    lax.fori_loop(0, STEPS, step, 0)

def trail(p, q, k, lx, ly, tiles):
    def rows(ref, first):
        t = ref[k].reshape(512, B)
        return split(jnp.concatenate([jnp.where(first > k, t[:B], 0.0), t[B:]], 0))
    xh, xl = rows(lx, p)
    yh, yl = rows(ly, q)
    for a in range(2):
        tiles[a] = tiles[a] - nt3(xh[B * a:B * a + B], xl[B * a:B * a + B], yh, yl)

def put_out(q, lx, tiles, out_ref):
    @pl.when(q < STEPS)
    def _():
        tiles[:, :, :B] = lx[jnp.minimum(q, STEPS - 1)]
    for a in range(2):
        for j in range(4):
            out_ref[pl.ds(4 * B * a + j, B, stride=4), :] = tiles[a, :, 128 * j:128 * j + 128]

def scratch():
    V = pltpu.VMEM
    return [V((STEPS, SLOTS, B, B), BF16), V((STEPS, SLOTS, B, B), BF16), V((B, B), BF16), V((B, B), BF16),
            V((4, 4, 64, 128), F32), V((4, 64, 128), F32), V((4, 4, 64, 128), F32), V((320, B), F32)]
MESH = pl.DeviceIdType.MESH
HOME = 1

class Comm:
    def __init__(self, p, q, own, g, lx, ly, send_sem, g_sem, x_sem, d_sem, in_sem, out_sem, z_sem, s_sem, y_sem):
        self.p, self.q, self.own, self.g, self.lx, self.ly = p, q, own, g, lx, ly
        self.px, self.py, self.pz, self.c = p % 4, p // 4, q // 2, q % 2
        self.send_sem, self.g_sem, self.x_sem, self.d_sem = send_sem, g_sem, x_sem, d_sem
        self.in_sem, self.out_sem = in_sem, out_sem
        self.z_sem, self.s_sem, self.y_sem = z_sem, s_sem, y_sem
        self.base, self.next, self.waiting = self.layout()[0], 0, False
        self.home = self.pz == HOME

    def at_z(self, d):
        return (self.p, 2 * ((self.pz + d) % 8) + self.c)

    def at_y(self, d):
        return (4 * ((self.py + d) % 4) + self.px, self.q)

    def at_x(self, d):
        return (4 * self.py + (self.px + d) % 4, self.q)

    def sibling(self):
        return (self.p, 2 * self.pz + 1 - self.c)

    def barrier(self):
        b = pltpu.get_barrier_semaphore()
        peers = [self.at_z(d) for d in (1, -1, 2, -2)] + [self.at_y(1), self.at_y(-1), self.at_x(1), self.at_x(-1), self.sibling()]
        for d in peers:
            pl.semaphore_signal(b, inc=1, device_id=d, device_id_type=MESH)
        pl.semaphore_wait(b, len(peers))

    def copy(self, cond, src, dst, send_sem, recv_sem, to):
        c = pltpu.make_async_remote_copy(src_ref=src, dst_ref=dst, send_sem=send_sem, recv_sem=recv_sem,
                                         device_id=to, device_id_type=MESH)
        pl.when(cond)(c.wait_send if self.waiting else c.start)

    def send(self, cond, src, dst, sem, to):
        self.copy(cond, src, dst, self.send_sem.at[self.next], sem, to)
        self.next += 1

    def take(self, cond, ref, sem):
        if self.waiting:
            return
        c = pltpu.make_async_remote_copy(src_ref=ref, dst_ref=ref, send_sem=self.send_sem.at[0],
                                         recv_sem=sem, device_id=self.sibling(), device_id_type=MESH)
        pl.when(cond)(c.wait_recv)

    @staticmethod
    def count(name, args):
        if name == "arrive":
            return 8 if args[1] == 0 else 0
        if name == "x_sibling":
            return 1
        if name == "y_forward":
            return 4
        return len(args[1]) * {"x_send": 9, "x_forward": 4, "finish": 3}[name]

    @classmethod
    def layout(cls):
        every = list(cls.BEGIN) + [op for n in sorted(cls.SCHEDULE) for op in cls.SCHEDULE[n]]
        base, at = {}, 0
        for name, *args in every:
            base[name, tuple(args)] = at
            at += cls.count(name, args)
        return base, at

    def do(self, name, *args):
        self.next = self.base[name, args]
        getattr(self, name)(*args)
        assert self.next <= self.base[name, args] + self.count(name, args), (name, args)

    def drain(self, name, *args):
        self.waiting = True
        self.do(name, *args)
        self.waiting = False

    def local(self, tiles):
        def half(a, j):
            return self.own[pl.ds(4 * B * a + j, B, stride=4), :]

        for a in range(2):
            for j in range(4):
                tiles[a, :, 128 * j:128 * j + 128] = half(a, j)

        @pl.when(self.q < 8)
        def _():
            k = jnp.minimum(self.q, 7)
            for a in range(2):
                for j in range(2):
                    self.g[k, 8 + a, :, 128 * j:128 * j + 128] = half(a, j)

    def gp(self, k, slot, piece):
        return self.g.at[k, slot, pl.ds(64 * piece, 64)]

    def to_home(self):
        k = jnp.minimum(self.q, 7)
        for a in range(2):
            for piece in range(4):
                ref = self.gp(k, 8 + a, piece)
                self.copy((self.q < 8) & (self.pz != HOME), ref, ref, self.in_sem.at[a, piece],
                          self.g_sem.at[k, 8 + a, piece], (self.p, 2 * HOME + self.c))

    def arrive(self, zs, a):
        k = 2 * zs + self.c
        for piece in range(4):
            ref, sem = self.gp(k, 8 + a, piece), self.g_sem.at[k, 8 + a, piece]
            if zs != HOME:
                self.take(k < 8, ref, sem)
            if a == 0:
                row = (self.p < 8) & (k <= self.p)
                pp = jnp.minimum(self.p, 7)
                for e in (1, -1):
                    self.send(row, ref, self.gp(k, pp, piece), self.g_sem.at[k, pp, piece], self.at_y(e))

    def x_sibling(self, zs, a):
        k = 2 * zs + self.c
        self.send(k < 8, self.g.at[k, 8 + a], self.g.at[k, 8 + a], self.x_sem.at[k, a], self.sibling())

    def y_forward(self, i):
        k = 2 * i + self.c
        for d, pieces in ((1, (0, 1)), (-1, (2, 3))):
            ys = (self.py - d) % 4
            r = jnp.minimum(4 * ys + self.px, 7)
            on = (ys < 2) & (k <= r)
            for piece in pieces:
                ref, sem = self.gp(k, r, piece), self.g_sem.at[k, r, piece]
                self.take(on, ref, sem)
                self.send(on, ref, ref, sem, self.at_y(d))

    def x_send(self, i, rows):
        k = 2 * i + self.c
        for ys in rows:
            r = 4 * ys + self.px
            dist = (self.py - ys) % 4
            for piece in range(4):
                rest = (dist == 2) | (dist == (1 if piece >= 2 else 3))
                ref, sem = self.gp(k, r, piece), self.g_sem.at[k, r, piece]
                self.take(rest & (k <= r), ref, sem)
                for e in (1, -1):
                    self.send(k <= r, self.gp(k, jnp.where(r == self.p, 8, r), piece), ref, sem, self.at_x(e))
            self.send((k <= r) & (dist != 0), self.g.at[k, r], self.g.at[k, r], self.d_sem.at[k, r], self.sibling())

    def x_forward(self, i, rows):
        k = 2 * i + self.c
        for d, pieces in ((1, (0, 1)), (-1, (2, 3))):
            xs = (self.px - d) % 4
            for ys in rows:
                r = 4 * ys + xs
                for piece in pieces:
                    ref, sem = self.gp(k, r, piece), self.g_sem.at[k, r, piece]
                    self.take(k <= r, ref, sem)
                    self.send(k <= r, ref, ref, sem, self.at_x(d))

    def finish(self, i, rows):
        k = 2 * i + self.c
        for dx, pieces in ((1, (2, 3)), (3, (0, 1)), (2, (0, 1, 2, 3))):
            xs = (self.px - dx) % 4
            for ys in rows:
                r = 4 * ys + xs
                for piece in pieces:
                    self.take(k <= r, self.gp(k, r, piece), self.g_sem.at[k, r, piece])
                self.send(k <= r, self.g.at[k, r], self.g.at[k, r], self.d_sem.at[k, r], self.sibling())

    def from_sibling(self, i, rows):
        k = 2 * i + 1 - self.c
        if 0 in rows:
            self.take(k < 8, self.g.at[k, 8], self.x_sem.at[k, 0])
        for r in rows:
            self.take((k <= r) & (r != self.p), self.g.at[k, r], self.d_sem.at[k, r])
        if 7 in rows:
            self.take(k < 8, self.g.at[k, 9], self.x_sem.at[k, 1])

    BEGIN = [("arrive", 0, 0), ("x_sibling", 0, 0), ("y_forward", 0), ("arrive", 1, 0), ("x_send", 0, (0,)),
             ("x_forward", 0, (0,)), ("x_send", 0, (1,)), ("y_forward", 1), ("finish", 0, (0,))]

    SCHEDULE = {
        0: [("x_sibling", 1, 0), ("arrive", 2, 0), ("arrive", 0, 1), ("x_sibling", 0, 1)],
        1: [("x_forward", 0, (1,)), ("x_send", 1, (0,)), ("y_forward", 2)],
        2: [("x_send", 1, (1,))],
        3: [("finish", 0, (1,)), ("x_sibling", 2, 0), ("arrive", 3, 0)],
        4: [("x_forward", 1, (0,)), ("x_send", 2, (0,))],
        5: [("x_forward", 1, (1,)), ("x_send", 2, (1,)), ("y_forward", 3)],
        6: [("x_sibling", 3, 0), ("arrive", 1, 1), ("x_sibling", 1, 1)],
        7: [("finish", 1, (0, 1))],
        8: [("x_forward", 2, (0, 1)), ("x_send", 3, (0, 1))],
        9: [("arrive", 2, 1), ("x_sibling", 2, 1)],
        10: [("arrive", 3, 1), ("x_sibling", 3, 1)],
        11: [("finish", 2, (0, 1))],
        13: [("x_forward", 3, (0, 1))],
        17: [("finish", 3, (0, 1))],
    }

    def begin(self):
        for op in self.BEGIN:
            self.do(*op)

    def pump(self, k, g):
        it = 4 * k + g
        for top in range(0, 20, 4):
            @pl.when(k == top // 4)
            def _():
                for n in range(top, top + 4):
                    if n in self.SCHEDULE:
                        @pl.when(it == n)
                        def _():
                            for op in self.SCHEDULE[n]:
                                self.do(*op)

        @pl.when((g == 0) & (k >= 1))
        def _():
            self.z_pass(k - 1)
            self.source_rest(k - 1)

        @pl.when((g == 1) & (k >= 2))
        def _():
            self.u_pass(k - 2)

        @pl.when((g == 3) & (k >= 3))
        def _():
            self.v_pass(k - 3)

    def fill(self, i):
        row = jnp.minimum(self.p, 7)
        for col in (2 * i, 2 * i + 1):
            @pl.when((self.p < 8) & (col <= self.p))
            def _():
                self.g[col, row] = self.g[col, 8]

    def drain_item(self, i):
        for name, args in self.base:
            if args[0] == i:
                self.drain(name, *args)

    def ready(self, k):
        @pl.when(k == 0)
        def _():
            self.from_sibling(0, range(4))
            self.fill(0)

        for i, at in ((0, 1), (1, 2), (2, 3), (3, 5)):
            @pl.when(k == at)
            def _():
                if i > 0:
                    self.from_sibling(i, range(8))
                    self.fill(i)
                self.drain_item(i)

    def ready_rest(self, k):
        @pl.when(k == 0)
        def _():
            self.from_sibling(0, range(4, 8))

    def z_pass(self, k):
        dist = (self.pz - HOME) % 8
        for n in range(4):
            ref = self.lx.at[k, self.c, pl.ds(64 * n, 64)]
            self.take(dist != 0, ref, self.z_sem.at[k, n])
            self.copy(dist < 4, ref, ref, self.out_sem.at[k, n], self.z_sem.at[k, n], self.at_z(1))
            self.copy((dist == 0) | (dist > 5), ref, ref, self.out_sem.at[k, 4 + n], self.z_sem.at[k, n], self.at_z(-1))
            self.source(k, self.c, n, 0)

    def s_send(self, k):
        ref = self.lx.at[k, self.c]
        self.copy(self.pz != HOME, ref, ref, self.out_sem.at[k, 8], self.s_sem.at[k], self.sibling())

    def s_take(self, k):
        self.take(self.pz != HOME, self.lx.at[k, 1 - self.c], self.s_sem.at[k])

    def plane(self):
        first = self.c == 0
        u = lambda d: (jnp.where(first, 4 * ((self.py + d) % 4) + self.px, 4 * self.py + (self.px + d) % 4), self.q)
        v = lambda d: (jnp.where(first, 4 * self.py + (self.px + d) % 4, 4 * ((self.py + d) % 4) + self.px), self.q)
        y, x = (self.py - self.q // 4) % 4, (self.px - self.q % 4) % 4
        return u, v, jnp.where(first, y, x), jnp.where(first, x, y)

    def part(self, ref, k, a, n):
        return ref.at[k, a, pl.ds(64 * n, 64)]

    def source(self, k, a, n, half):
        u, v, _, _ = self.plane()
        for e, to in enumerate((u(1), u(-1), v(1), v(-1))):
            self.copy(self.p == self.q, self.part(self.lx, k, a, n), self.part(self.ly, k, a, n),
                      self.out_sem.at[k, 9 + 16 * half + 4 * n + e], self.y_sem.at[k, a, n], to)

    def source_rest(self, k):
        for n in range(4):
            self.source(k, 1 - self.c, n, 1)

    def u_pass(self, k):
        u, v, du, dv = self.plane()
        line = (dv == 0) & (du != 0)
        for half in range(2):
            a = self.c if half == 0 else 1 - self.c
            for n in range(4):
                ref, sem = self.part(self.ly, k, a, n), self.y_sem.at[k, a, n]
                self.take(line, ref, sem)
                at = 9 + 12 * half + 3 * n
                self.copy(line, ref, ref, self.out_sem.at[k, at], sem, v(1))
                self.copy(line, ref, ref, self.out_sem.at[k, at + 1], sem, v(-1))
                self.copy(line & (du == (1 if n < 2 else 3)), ref, ref, self.out_sem.at[k, at + 2], sem, u(1 if n < 2 else -1))

    def v_pass(self, k):
        u, v, du, dv = self.plane()
        for half in range(2):
            a = self.c if half == 0 else 1 - self.c
            for n in range(4):
                ref, sem = self.part(self.ly, k, a, n), self.y_sem.at[k, a, n]
                self.take(dv != 0, ref, sem)
                self.copy(dv == (1 if n < 2 else 3), ref, ref, self.out_sem.at[k, 9 + 4 * half + n], sem, v(1 if n < 2 else -1))

        @pl.when((self.p == self.q) & (not self.waiting))
        def _():
            self.ly[k] = self.lx[k]

    def end(self):
        @pl.when(self.home)
        def _():
            for name, args in self.base:
                if args[0] not in (0, 1, 2, 3):
                    self.drain(name, *args)

        self.waiting = True
        self.to_home()

        def one(k, _):
            self.z_pass(k)
            self.s_send(k)
            self.source_rest(k)
            self.u_pass(k)
            self.v_pass(k)
            return 0
        lax.fori_loop(0, STEPS, one, 0)
        self.waiting = False

def comm_scratch():
    D = pltpu.SemaphoreType.DMA
    return [D((Comm.layout()[1],)), D((8, 10, 4)), D((8, 2)), D((8, 8)), D((2, 4)), D((8, 41)), D((8, 4)), D((8,)), D((8, 2, 4))]

from jax.sharding import PartitionSpec as P


def entry(own, out_ref, g, lx, ly, tiles, *rest):
    p, q = lax.axis_index("row"), lax.axis_index("col")
    n = len(comm_scratch())
    comm = Comm(p, q, own, g, lx, ly, *rest[:n])
    comm.local(tiles)
    comm.barrier()
    comm.to_home()

    @pl.when(comm.home)
    def _():
        comm.begin()
        lead_factor(p, g, lx, *rest[n:], comm.ready, comm.ready_rest, comm.pump)
        comm.z_pass(7)
        comm.source_rest(7)
        comm.u_pass(6)
        comm.v_pass(5)

        def old(k, _):
            trail(p, q, k, lx, ly, tiles)
            return 0
        lax.fori_loop(0, 6, old, 0)
        comm.u_pass(7)
        comm.v_pass(6)
        trail(p, q, 6, lx, ly, tiles)

    @pl.when(jnp.logical_not(comm.home))
    def _():
        def turn(n, _):
            @pl.when(n < 8)
            def _():
                comm.z_pass(n)
                comm.s_send(n)
                comm.s_take(n)
                comm.source_rest(n)

            @pl.when((n >= 1) & (n < 9))
            def _():
                comm.u_pass(n - 1)

            @pl.when((n >= 2) & (n < 9))
            def _():
                comm.v_pass(n - 2)
                trail(p, q, n - 2, lx, ly, tiles)
            return 0
        lax.fori_loop(0, 9, turn, 0)

    comm.v_pass(7)
    trail(p, q, 7, lx, ly, tiles)
    put_out(q, lx, tiles, out_ref)
    comm.end()


def on_device(matrix):
    out = pl.pallas_call(
        entry,
        out_shape=jax.ShapeDtypeStruct((8 * B, 128), F32),
        in_specs=[pl.BlockSpec(memory_space=pltpu.VMEM)],
        out_specs=pl.BlockSpec(memory_space=pltpu.VMEM),
        scratch_shapes=[pltpu.VMEM((STEPS, SLOTS, B, B), F32), pltpu.VMEM((STEPS, 2, B, B), F32),
                        pltpu.VMEM((STEPS, 2, B, B), F32), pltpu.VMEM((2, B, 2 * B), F32)] + comm_scratch() + scratch(),
        compiler_params=pltpu.CompilerParams(vmem_limit_bytes=63 * 1024 * 1024, collective_id=0, has_side_effects=True),
        name="steps",
    )(matrix.reshape(8 * B, 128))
    return out.reshape(matrix.shape)


def solution(mesh):
    spec = P(None, "row", None, None, "col", None)
    return jax.shard_map(on_device, mesh=mesh, in_specs=(spec,), out_specs=spec, check_vma=False)
```

```python
import jax, jax.numpy as jnp, functools
from jax import lax
from jax.experimental import pallas as pl
from jax.experimental.pallas import tpu as pltpu

F32, BF16 = jnp.float32, jnp.bfloat16

def over_lanes(v, c):
    return jnp.broadcast_to(v[:, c:c + 1], (8, 128))

def over_rows(v, r):
    return jnp.broadcast_to(v[r:r + 1, :], (8, 128))

def eliminate(rows):
    sub = lax.broadcasted_iota(jnp.int32, (8, 128), 0)
    rows = list(rows)
    diag = [over_lanes(rows[0], t) for t in range(8)]
    for s in range(8):
        off = {i: [over_lanes(rows[i], 8 * s + m) for m in range(8)] for i in range(s + 1, 8)}
        nxt = [over_lanes(rows[s + 1], 8 * (s + 1) + t) for t in range(8)] if s < 7 else None
        top = rows[s]
        for m in range(8):
            root = lax.rsqrt(over_rows(diag[m], m))
            lead = diag[m] * root
            unit = over_rows(top, m) * root
            top = jnp.where(sub == m, unit, top - jnp.where(sub > m, lead, 0.0) * unit)
            scal = {t: over_rows(lead, t) for t in range(m + 1, 8)}
            for t in range(m + 1, 8):
                diag[t] = diag[t] - lead * scal[t]
            for i in range(s + 1, 8):
                mult = off[i][m] * root
                for t in range(m + 1, 8):
                    off[i][t] = off[i][t] - mult * scal[t]
                rows[i] = rows[i] - mult * unit
                if i == s + 1:
                    for t in range(8):
                        nxt[t] = nxt[t] - mult * over_rows(mult, t)
        rows[s] = top
        diag = nxt
    return rows

def split(x):
    hi = x.astype(BF16)
    return hi, (x - hi.astype(F32)).astype(BF16)

def nt(a, b):
    return lax.dot_general(a, b, (((1,), (1,)), ((), ())), preferred_element_type=F32)

def nn(a, b):
    return lax.dot_general(a, b, (((1,), (0,)), ((), ())), preferred_element_type=F32)

def factor_tile(tb, ud, lb, zpad, w_hi, w_lo, before=None, beside=None):
    low = lax.broadcasted_iota(jnp.int32, (64, 128), 1) < 64
    eye = jnp.where(
        lax.broadcasted_iota(jnp.int32, (64, 128), 1)
        == lax.broadcasted_iota(jnp.int32, (64, 128), 0) + 64, 1.0, 0.0).astype(F32)
    zpad[...] = jnp.zeros_like(zpad)

    def group(g, _):
        if before is not None:
            before(g)
        if beside is not None:
            beside(g)
        block = jnp.where(low, tb[g, g], eye)
        done = eliminate([block[8 * i:8 * i + 8] for i in range(8)])
        m = jnp.concatenate(done, 0)
        ud[g] = m
        wz = jnp.where(low, 0.0, m)
        wz_hi, wz_lo = split(wz)
        tcol = tb[:, g].reshape(256, 128)
        t_hi, t_lo = split(tcol)
        w2_hi = jnp.concatenate([wz_hi, wz_hi], 0)
        w2_lo = jnp.concatenate([wz_lo, wz_lo], 0)
        p = nt(jnp.concatenate([t_hi, t_lo], 1), jnp.concatenate([w2_hi, w2_hi], 1)) + nt(t_hi, w2_lo)
        rowblk = lax.broadcasted_iota(jnp.int32, (256, 128), 0) // 64
        p = jnp.where(rowblk > g, p, 0.0)
        lb[:, g] = p.reshape(4, 64, 128)
        hi = p.astype(BF16)
        hif = hi.astype(F32)
        lof = p - hif
        lo = lof.astype(BF16)
        lowp = lax.broadcasted_iota(jnp.int32, (256, 128), 1) < 64
        lhs = jnp.concatenate([jnp.where(lowp, hif, lof).astype(BF16),
                               jnp.where(lowp, hif, 0.0).astype(BF16)], 1)
        for h in range(2):
            parts = []
            for j in (2 * h, 2 * h + 1):
                pj = jnp.concatenate([hi[64 * j:64 * j + 64], lo[64 * j:64 * j + 64]], 1)
                parts += [pj, pj]
            upd = nt(lhs, jnp.concatenate(parts, 0))
            for j in range(2):
                tb[:, 2 * h + j] = tb[:, 2 * h + j] - upd[:, 128 * j:128 * j + 128].reshape(4, 64, 128)
        z = zpad[pl.ds(pl.multiple_of(64 * g, 64), 128), :]
        z_hi, z_lo = split(z)
        mix = nn(jnp.concatenate([wz_hi, wz_lo], 1), jnp.concatenate([z_hi, z_hi], 0)) + nn(wz_hi, z_lo)
        turned = pltpu.roll(m, 64, 1)
        both = jnp.where(low, turned, m)
        here = lax.broadcasted_iota(jnp.int32, (64, 256), 1) // 64 == g
        wrow = jnp.where(here, jnp.concatenate([both, both], 1), -mix)
        at = pl.ds(pl.multiple_of(64 * g, 64), 64)
        r_hi, r_lo = split(wrow)
        w_hi[at, :] = r_hi
        w_lo[at, :] = r_lo
        zpad[64:, :] = zpad[64:, :] + nn(lhs, jnp.concatenate([r_hi, r_hi, r_lo, r_lo], 0))
        return 0
    for g in range(4):
        group(g, 0)

def blocks(tile, tb):
    low = lax.broadcasted_iota(jnp.int32, (256, 128), 1) < 64
    for h in range(2):
        x = tile[:, 128 * h:128 * h + 128]
        r = pltpu.roll(x, 64, 1)
        tb[:, 2 * h] = jnp.where(low, x, r).reshape(4, 64, 128)
        tb[:, 2 * h + 1] = jnp.where(low, r, x).reshape(4, 64, 128)


B = 256
STEPS = 8
SLOTS = 10

def nt3(ah, al, bh, bl):
    return nt(ah, bh) + nt(ah, bl) + nt(al, bh)

def nn3(ah, al, bh, bl):
    return nn(ah, bh) + nn(ah, bl) + nn(al, bh)

def pair(r):
    return pl.ds(2 * r, 2)

def lead_factor(p, g, lx, lh, ll, wh, wl, tb, ud, lb, zpad, ready, ready_rest, pump):
    def apply(j, r, m):
        got = nt3(lh[m, pair(r)].reshape(512, B), ll[m, pair(r)].reshape(512, B), lh[m, j], ll[m, j])
        g[j, pair(r)] = g[j, pair(r)] - got.reshape(2, B, B)

    def step(k, _):
        ready(k)

        def last(r, _):
            def term(m, _):
                apply(k, r, m)
                return 0
            return lax.fori_loop(jnp.where(k == 2, 0, k - 1), k, term, 0)
        lax.fori_loop(jnp.where(k > 0, k // 2, 5), jnp.where(k > 0, k // 2 + 1, 5), last, 0)
        blocks(g[k, k], tb)

        def beside(i):
            below = 4 - k // 2
            now = below * jnp.where(k == 0, 0, jnp.where(k == 2, 2, 1))
            j = k + 1
            rows = jnp.maximum(5 - j // 2, 1)
            for n in range(4):
                turn = 4 * i + n
                first = turn < now
                later = jnp.maximum(turn - now, 0)
                m = later // rows
                on = (m < k) & (j < STEPS) & (j != 2)
                apply(jnp.where(first, k, jnp.where(on, j, 7)),
                      jnp.where(first, k // 2 + 1 + turn % below, jnp.where(on, j // 2 + later % rows, 0)),
                      jnp.where(first, jnp.where(k == 2, turn // below, k - 1), jnp.where(on, m, 0)))

        factor_tile(tb, ud, lb, zpad, wh, wl, lambda i: pump(k, i), beside)
        ready_rest(k)

        def solve(r):
            ah, al = split(g[k, pair(r)].reshape(512, B))
            return nt3(ah, al, wh[...], wl[...])

        def keep(r, got):
            hi, lo = split(got.reshape(2, B, B))
            lh[k, pair(r)] = hi
            ll[k, pair(r)] = lo

        got = solve(4)
        got = jnp.concatenate([jnp.where(p > k, got[:B], 0.0), got[B:]], 0)
        keep(4, got)
        lx[k] = got.reshape(2, B, B)

        @pl.when(p == k)
        def _():
            low = lax.broadcasted_iota(jnp.int32, (64, 128), 1) < 64
            tri = lax.broadcasted_iota(jnp.int32, (64, 128), 0) <= lax.broadcasted_iota(jnp.int32, (64, 128), 1)
            for i in range(4):
                up = jnp.where(tri & low, ud[i], 0.0)
                turned = jnp.concatenate([up, jnp.zeros((64, 128), F32)], 0).T[:64]
                twice = turned + pltpu.roll(turned, 64, 1)
                parts = [lb[i, j] if j < i else (twice if j == i else jnp.zeros((64, 128), F32)) for j in range(4)]
                for h in range(2):
                    lx[k, 0, 64 * i:64 * i + 64, 128 * h:128 * h + 128] = jnp.where(low, parts[2 * h], parts[2 * h + 1])

        def rest(r, _):
            keep(r, solve(r))
            return 0
        lax.fori_loop((k + 1) // 2, 4, rest, 0)
        return 0
    lax.fori_loop(0, STEPS, step, 0)

def trail(p, q, k, lx, ly, tiles):
    def rows(ref, first):
        t = ref[k].reshape(512, B)
        return split(jnp.concatenate([jnp.where(first > k, t[:B], 0.0), t[B:]], 0))
    xh, xl = rows(lx, p)
    yh, yl = rows(ly, q)
    for a in range(2):
        tiles[a] = tiles[a] - nt3(xh[B * a:B * a + B], xl[B * a:B * a + B], yh, yl)

def put_out(q, lx, tiles, out_ref):
    @pl.when(q < STEPS)
    def _():
        tiles[:, :, :B] = lx[jnp.minimum(q, STEPS - 1)]
    for a in range(2):
        for j in range(4):
            out_ref[pl.ds(4 * B * a + j, B, stride=4), :] = tiles[a, :, 128 * j:128 * j + 128]

def scratch():
    V = pltpu.VMEM
    return [V((STEPS, SLOTS, B, B), BF16), V((STEPS, SLOTS, B, B), BF16), V((B, B), BF16), V((B, B), BF16),
            V((4, 4, 64, 128), F32), V((4, 64, 128), F32), V((4, 4, 64, 128), F32), V((320, B), F32)]
MESH = pl.DeviceIdType.MESH
HOME = 1

class Comm:
    def __init__(self, p, q, own, g, lx, ly, send_sem, g_sem, x_sem, d_sem, in_sem, out_sem, z_sem, s_sem, y_sem):
        self.p, self.q, self.own, self.g, self.lx, self.ly = p, q, own, g, lx, ly
        self.px, self.py, self.pz, self.c = p % 4, p // 4, q // 2, q % 2
        self.send_sem, self.g_sem, self.x_sem, self.d_sem = send_sem, g_sem, x_sem, d_sem
        self.in_sem, self.out_sem = in_sem, out_sem
        self.z_sem, self.s_sem, self.y_sem = z_sem, s_sem, y_sem
        self.base, self.next, self.waiting = self.layout()[0], 0, False
        self.home = self.pz == HOME

    def at_z(self, d):
        return (self.p, 2 * ((self.pz + d) % 8) + self.c)

    def at_y(self, d):
        return (4 * ((self.py + d) % 4) + self.px, self.q)

    def at_x(self, d):
        return (4 * self.py + (self.px + d) % 4, self.q)

    def sibling(self):
        return (self.p, 2 * self.pz + 1 - self.c)

    def barrier(self):
        b = pltpu.get_barrier_semaphore()
        peers = [self.at_z(d) for d in (1, -1, 2, -2)] + [self.at_y(1), self.at_y(-1), self.at_x(1), self.at_x(-1), self.sibling()]
        for d in peers:
            pl.semaphore_signal(b, inc=1, device_id=d, device_id_type=MESH)
        pl.semaphore_wait(b, len(peers))

    def copy(self, cond, src, dst, send_sem, recv_sem, to):
        c = pltpu.make_async_remote_copy(src_ref=src, dst_ref=dst, send_sem=send_sem, recv_sem=recv_sem,
                                         device_id=to, device_id_type=MESH)
        pl.when(cond)(c.wait_send if self.waiting else c.start)

    def send(self, cond, src, dst, sem, to):
        self.copy(cond, src, dst, self.send_sem.at[self.next], sem, to)
        self.next += 1

    def take(self, cond, ref, sem):
        if self.waiting:
            return
        c = pltpu.make_async_remote_copy(src_ref=ref, dst_ref=ref, send_sem=self.send_sem.at[0],
                                         recv_sem=sem, device_id=self.sibling(), device_id_type=MESH)
        pl.when(cond)(c.wait_recv)

    @staticmethod
    def count(name, args):
        if name == "arrive":
            return 8 if args[1] == 0 else 0
        if name == "x_sibling":
            return 1
        if name == "y_forward":
            return 4
        return len(args[1]) * {"x_send": 9, "x_forward": 4, "finish": 3}[name]

    @classmethod
    def layout(cls):
        every = list(cls.BEGIN) + [op for n in sorted(cls.SCHEDULE) for op in cls.SCHEDULE[n]]
        base, at = {}, 0
        for name, *args in every:
            base[name, tuple(args)] = at
            at += cls.count(name, args)
        return base, at

    def do(self, name, *args):
        self.next = self.base[name, args]
        getattr(self, name)(*args)
        assert self.next <= self.base[name, args] + self.count(name, args), (name, args)

    def drain(self, name, *args):
        self.waiting = True
        self.do(name, *args)
        self.waiting = False

    def local(self, tiles):
        def half(a, j):
            return self.own[pl.ds(4 * B * a + j, B, stride=4), :]

        for a in range(2):
            for j in range(4):
                tiles[a, :, 128 * j:128 * j + 128] = half(a, j)

        @pl.when(self.q < 8)
        def _():
            k = jnp.minimum(self.q, 7)
            for a in range(2):
                for j in range(2):
                    self.g[k, 8 + a, :, 128 * j:128 * j + 128] = half(a, j)

    def gp(self, k, slot, piece):
        return self.g.at[k, slot, pl.ds(64 * piece, 64)]

    def to_home(self):
        k = jnp.minimum(self.q, 7)
        for a in range(2):
            for piece in range(4):
                ref = self.gp(k, 8 + a, piece)
                self.copy((self.q < 8) & (self.pz != HOME), ref, ref, self.in_sem.at[a, piece],
                          self.g_sem.at[k, 8 + a, piece], (self.p, 2 * HOME + self.c))

    def arrive(self, zs, a):
        k = 2 * zs + self.c
        for piece in range(4):
            ref, sem = self.gp(k, 8 + a, piece), self.g_sem.at[k, 8 + a, piece]
            if zs != HOME:
                self.take(k < 8, ref, sem)
            if a == 0:
                row = (self.p < 8) & (k <= self.p)
                pp = jnp.minimum(self.p, 7)
                for e in (1, -1):
                    self.send(row, ref, self.gp(k, pp, piece), self.g_sem.at[k, pp, piece], self.at_y(e))

    def x_sibling(self, zs, a):
        k = 2 * zs + self.c
        self.send(k < 8, self.g.at[k, 8 + a], self.g.at[k, 8 + a], self.x_sem.at[k, a], self.sibling())

    def y_forward(self, i):
        k = 2 * i + self.c
        for d, pieces in ((1, (0, 1)), (-1, (2, 3))):
            ys = (self.py - d) % 4
            r = jnp.minimum(4 * ys + self.px, 7)
            on = (ys < 2) & (k <= r)
            for piece in pieces:
                ref, sem = self.gp(k, r, piece), self.g_sem.at[k, r, piece]
                self.take(on, ref, sem)
                self.send(on, ref, ref, sem, self.at_y(d))

    def x_send(self, i, rows):
        k = 2 * i + self.c
        for ys in rows:
            r = 4 * ys + self.px
            dist = (self.py - ys) % 4
            for piece in range(4):
                rest = (dist == 2) | (dist == (1 if piece >= 2 else 3))
                ref, sem = self.gp(k, r, piece), self.g_sem.at[k, r, piece]
                self.take(rest & (k <= r), ref, sem)
                for e in (1, -1):
                    self.send(k <= r, self.gp(k, jnp.where(r == self.p, 8, r), piece), ref, sem, self.at_x(e))
            self.send((k <= r) & (dist != 0), self.g.at[k, r], self.g.at[k, r], self.d_sem.at[k, r], self.sibling())

    def x_forward(self, i, rows):
        k = 2 * i + self.c
        for d, pieces in ((1, (0, 1)), (-1, (2, 3))):
            xs = (self.px - d) % 4
            for ys in rows:
                r = 4 * ys + xs
                for piece in pieces:
                    ref, sem = self.gp(k, r, piece), self.g_sem.at[k, r, piece]
                    self.take(k <= r, ref, sem)
                    self.send(k <= r, ref, ref, sem, self.at_x(d))

    def finish(self, i, rows):
        k = 2 * i + self.c
        for dx, pieces in ((1, (2, 3)), (3, (0, 1)), (2, (0, 1, 2, 3))):
            xs = (self.px - dx) % 4
            for ys in rows:
                r = 4 * ys + xs
                for piece in pieces:
                    self.take(k <= r, self.gp(k, r, piece), self.g_sem.at[k, r, piece])
                self.send(k <= r, self.g.at[k, r], self.g.at[k, r], self.d_sem.at[k, r], self.sibling())

    def from_sibling(self, i, rows):
        k = 2 * i + 1 - self.c
        if 0 in rows:
            self.take(k < 8, self.g.at[k, 8], self.x_sem.at[k, 0])
        for r in rows:
            self.take((k <= r) & (r != self.p), self.g.at[k, r], self.d_sem.at[k, r])
        if 7 in rows:
            self.take(k < 8, self.g.at[k, 9], self.x_sem.at[k, 1])

    BEGIN = [("arrive", 0, 0), ("x_sibling", 0, 0), ("y_forward", 0), ("arrive", 1, 0), ("x_send", 0, (0,)),
             ("x_forward", 0, (0,)), ("x_send", 0, (1,)), ("y_forward", 1), ("finish", 0, (0,))]

    SCHEDULE = {
        0: [("x_sibling", 1, 0), ("arrive", 2, 0), ("arrive", 0, 1), ("x_sibling", 0, 1)],
        1: [("x_forward", 0, (1,)), ("x_send", 1, (0,)), ("y_forward", 2)],
        2: [("x_send", 1, (1,))],
        3: [("finish", 0, (1,)), ("x_sibling", 2, 0), ("arrive", 3, 0)],
        4: [("x_forward", 1, (0,)), ("x_send", 2, (0,))],
        5: [("x_forward", 1, (1,)), ("x_send", 2, (1,)), ("y_forward", 3)],
        6: [("x_sibling", 3, 0), ("arrive", 1, 1), ("x_sibling", 1, 1)],
        7: [("finish", 1, (0, 1))],
        8: [("x_forward", 2, (0, 1)), ("x_send", 3, (0, 1))],
        9: [("arrive", 2, 1), ("x_sibling", 2, 1)],
        10: [("arrive", 3, 1), ("x_sibling", 3, 1)],
        11: [("finish", 2, (0, 1))],
        13: [("x_forward", 3, (0, 1))],
        17: [("finish", 3, (0, 1))],
    }

    def begin(self):
        for op in self.BEGIN:
            self.do(*op)

    def pump(self, k, g):
        it = 4 * k + g
        for top in range(0, 20, 4):
            @pl.when(k == top // 4)
            def _():
                for n in range(top, top + 4):
                    if n in self.SCHEDULE:
                        @pl.when(it == n)
                        def _():
                            for op in self.SCHEDULE[n]:
                                self.do(*op)

        @pl.when((g == 0) & (k >= 1))
        def _():
            self.z_pass(k - 1)
            self.source_rest(k - 1)

        @pl.when((g == 1) & (k >= 2))
        def _():
            self.u_pass(k - 2)

        @pl.when((g == 3) & (k >= 3))
        def _():
            self.v_pass(k - 3)

    def fill(self, i):
        row = jnp.minimum(self.p, 7)
        for col in (2 * i, 2 * i + 1):
            @pl.when((self.p < 8) & (col <= self.p))
            def _():
                self.g[col, row] = self.g[col, 8]

    def drain_item(self, i):
        for name, args in self.base:
            if args[0] == i:
                self.drain(name, *args)

    def ready(self, k):
        @pl.when(k == 0)
        def _():
            self.from_sibling(0, range(4))
            self.fill(0)

        for i, at in ((0, 1), (1, 2), (2, 3), (3, 5)):
            @pl.when(k == at)
            def _():
                if i > 0:
                    self.from_sibling(i, range(8))
                    self.fill(i)
                self.drain_item(i)

    def ready_rest(self, k):
        @pl.when(k == 0)
        def _():
            self.from_sibling(0, range(4, 8))

    def z_pass(self, k):
        dist = (self.pz - HOME) % 8
        for n in range(4):
            ref = self.lx.at[k, self.c, pl.ds(64 * n, 64)]
            self.take(dist != 0, ref, self.z_sem.at[k, n])
            self.copy(dist < 4, ref, ref, self.out_sem.at[k, n], self.z_sem.at[k, n], self.at_z(1))
            self.copy((dist == 0) | (dist > 5), ref, ref, self.out_sem.at[k, 4 + n], self.z_sem.at[k, n], self.at_z(-1))
            self.source(k, self.c, n, 0)

    def s_send(self, k):
        ref = self.lx.at[k, self.c]
        self.copy(self.pz != HOME, ref, ref, self.out_sem.at[k, 8], self.s_sem.at[k], self.sibling())

    def s_take(self, k):
        self.take(self.pz != HOME, self.lx.at[k, 1 - self.c], self.s_sem.at[k])

    def plane(self):
        first = self.c == 0
        u = lambda d: (jnp.where(first, 4 * ((self.py + d) % 4) + self.px, 4 * self.py + (self.px + d) % 4), self.q)
        v = lambda d: (jnp.where(first, 4 * self.py + (self.px + d) % 4, 4 * ((self.py + d) % 4) + self.px), self.q)
        y, x = (self.py - self.q // 4) % 4, (self.px - self.q % 4) % 4
        return u, v, jnp.where(first, y, x), jnp.where(first, x, y)

    def part(self, ref, k, a, n):
        return ref.at[k, a, pl.ds(64 * n, 64)]

    def source(self, k, a, n, half):
        u, v, _, _ = self.plane()
        for e, to in enumerate((u(1), u(-1), v(1), v(-1))):
            self.copy(self.p == self.q, self.part(self.lx, k, a, n), self.part(self.ly, k, a, n),
                      self.out_sem.at[k, 9 + 16 * half + 4 * n + e], self.y_sem.at[k, a, n], to)

    def source_rest(self, k):
        for n in range(4):
            self.source(k, 1 - self.c, n, 1)

    def u_pass(self, k):
        u, v, du, dv = self.plane()
        line = (dv == 0) & (du != 0)
        for half in range(2):
            a = self.c if half == 0 else 1 - self.c
            for n in range(4):
                ref, sem = self.part(self.ly, k, a, n), self.y_sem.at[k, a, n]
                self.take(line, ref, sem)
                at = 9 + 12 * half + 3 * n
                self.copy(line, ref, ref, self.out_sem.at[k, at], sem, v(1))
                self.copy(line, ref, ref, self.out_sem.at[k, at + 1], sem, v(-1))
                self.copy(line & (du == (1 if n < 2 else 3)), ref, ref, self.out_sem.at[k, at + 2], sem, u(1 if n < 2 else -1))

    def v_pass(self, k):
        u, v, du, dv = self.plane()
        for half in range(2):
            a = self.c if half == 0 else 1 - self.c
            for n in range(4):
                ref, sem = self.part(self.ly, k, a, n), self.y_sem.at[k, a, n]
                self.take(dv != 0, ref, sem)
                self.copy(dv == (1 if n < 2 else 3), ref, ref, self.out_sem.at[k, 9 + 4 * half + n], sem, v(1 if n < 2 else -1))

        @pl.when((self.p == self.q) & (not self.waiting))
        def _():
            self.ly[k] = self.lx[k]

    def end(self):
        @pl.when(self.home)
        def _():
            for name, args in self.base:
                if args[0] not in (0, 1, 2, 3):
                    self.drain(name, *args)

        self.waiting = True
        self.to_home()

        def one(k, _):
            self.z_pass(k)
            self.s_send(k)
            self.source_rest(k)
            self.u_pass(k)
            self.v_pass(k)
            return 0
        lax.fori_loop(0, STEPS, one, 0)
        self.waiting = False

def comm_scratch():
    D = pltpu.SemaphoreType.DMA
    return [D((Comm.layout()[1],)), D((8, 10, 4)), D((8, 2)), D((8, 8)), D((2, 4)), D((8, 41)), D((8, 4)), D((8,)), D((8, 2, 4))]

from jax.sharding import PartitionSpec as P


def entry(own, out_ref, g, lx, ly, tiles, *rest):
    p, q = lax.axis_index("row"), lax.axis_index("col")
    n = len(comm_scratch())
    comm = Comm(p, q, own, g, lx, ly, *rest[:n])
    comm.local(tiles)
    comm.barrier()
    comm.to_home()

    @pl.when(comm.home)
    def _():
        comm.begin()
        lead_factor(p, g, lx, *rest[n:], comm.ready, comm.ready_rest, comm.pump)
        comm.z_pass(7)
        comm.source_rest(7)
        comm.u_pass(6)
        comm.v_pass(5)

        def old(k, _):
            trail(p, q, k, lx, ly, tiles)
            return 0
        lax.fori_loop(0, 6, old, 0)
        comm.u_pass(7)
        comm.v_pass(6)
        trail(p, q, 6, lx, ly, tiles)

    @pl.when(jnp.logical_not(comm.home))
    def _():
        def turn(n, _):
            @pl.when(n < 8)
            def _():
                comm.z_pass(n)
                comm.s_send(n)
                comm.s_take(n)
                comm.source_rest(n)

            @pl.when((n >= 1) & (n < 9))
            def _():
                comm.u_pass(n - 1)

            @pl.when((n >= 2) & (n < 9))
            def _():
                comm.v_pass(n - 2)
                trail(p, q, n - 2, lx, ly, tiles)
            return 0
        lax.fori_loop(0, 9, turn, 0)

    comm.v_pass(7)
    trail(p, q, 7, lx, ly, tiles)
    put_out(q, lx, tiles, out_ref)
    comm.end()


def on_device(matrix):
    out = pl.pallas_call(
        entry,
        out_shape=jax.ShapeDtypeStruct((8 * B, 128), F32),
        in_specs=[pl.BlockSpec(memory_space=pltpu.VMEM)],
        out_specs=pl.BlockSpec(memory_space=pltpu.VMEM),
        scratch_shapes=[pltpu.VMEM((STEPS, SLOTS, B, B), F32), pltpu.VMEM((STEPS, 2, B, B), F32),
                        pltpu.VMEM((STEPS, 2, B, B), F32), pltpu.VMEM((2, B, 2 * B), F32)] + comm_scratch() + scratch(),
        compiler_params=pltpu.CompilerParams(vmem_limit_bytes=63 * 1024 * 1024, collective_id=0, has_side_effects=True),
        name="steps",
    )(matrix.reshape(8 * B, 128))
    return out.reshape(matrix.shape)


def solution(mesh):
    spec = P(None, "row", None, None, "col", None)
    return jax.shard_map(on_device, mesh=mesh, in_specs=(spec,), out_specs=spec, check_vma=False)
```

```python
import jax, jax.numpy as jnp, functools
from jax import lax
from jax.experimental import pallas as pl
from jax.experimental.pallas import tpu as pltpu

F32, BF16 = jnp.float32, jnp.bfloat16

def over_lanes(v, c):
    return jnp.broadcast_to(v[:, c:c + 1], (8, 128))

def over_rows(v, r):
    return jnp.broadcast_to(v[r:r + 1, :], (8, 128))

def eliminate(rows):
    sub = lax.broadcasted_iota(jnp.int32, (8, 128), 0)
    rows = list(rows)
    diag = [over_lanes(rows[0], t) for t in range(8)]
    for s in range(8):
        off = {i: [over_lanes(rows[i], 8 * s + m) for m in range(8)] for i in range(s + 1, 8)}
        nxt = [over_lanes(rows[s + 1], 8 * (s + 1) + t) for t in range(8)] if s < 7 else None
        top = rows[s]
        for m in range(8):
            root = lax.rsqrt(over_rows(diag[m], m))
            lead = diag[m] * root
            unit = over_rows(top, m) * root
            top = jnp.where(sub == m, unit, top - jnp.where(sub > m, lead, 0.0) * unit)
            scal = {t: over_rows(lead, t) for t in range(m + 1, 8)}
            for t in range(m + 1, 8):
                diag[t] = diag[t] - lead * scal[t]
            for i in range(s + 1, 8):
                mult = off[i][m] * root
                for t in range(m + 1, 8):
                    off[i][t] = off[i][t] - mult * scal[t]
                rows[i] = rows[i] - mult * unit
                if i == s + 1:
                    for t in range(8):
                        nxt[t] = nxt[t] - mult * over_rows(mult, t)
        rows[s] = top
        diag = nxt
    return rows

def split(x):
    hi = x.astype(BF16)
    return hi, (x - hi.astype(F32)).astype(BF16)

def nt(a, b):
    return lax.dot_general(a, b, (((1,), (1,)), ((), ())), preferred_element_type=F32)

def nn(a, b):
    return lax.dot_general(a, b, (((1,), (0,)), ((), ())), preferred_element_type=F32)

def factor_tile(tb, ud, lb, zpad, w_hi, w_lo, before=None, beside=None):
    low = lax.broadcasted_iota(jnp.int32, (64, 128), 1) < 64
    eye = jnp.where(
        lax.broadcasted_iota(jnp.int32, (64, 128), 1)
        == lax.broadcasted_iota(jnp.int32, (64, 128), 0) + 64, 1.0, 0.0).astype(F32)
    zpad[...] = jnp.zeros_like(zpad)

    def group(g, _):
        if before is not None:
            before(g)
        if beside is not None:
            beside(g)
        block = jnp.where(low, tb[g, g], eye)
        done = eliminate([block[8 * i:8 * i + 8] for i in range(8)])
        m = jnp.concatenate(done, 0)
        ud[g] = m
        wz = jnp.where(low, 0.0, m)
        wz_hi, wz_lo = split(wz)
        tcol = tb[:, g].reshape(256, 128)
        t_hi, t_lo = split(tcol)
        w2_hi = jnp.concatenate([wz_hi, wz_hi], 0)
        w2_lo = jnp.concatenate([wz_lo, wz_lo], 0)
        p = nt(jnp.concatenate([t_hi, t_lo], 1), jnp.concatenate([w2_hi, w2_hi], 1)) + nt(t_hi, w2_lo)
        rowblk = lax.broadcasted_iota(jnp.int32, (256, 128), 0) // 64
        p = jnp.where(rowblk > g, p, 0.0)
        lb[:, g] = p.reshape(4, 64, 128)
        hi = p.astype(BF16)
        hif = hi.astype(F32)
        lof = p - hif
        lo = lof.astype(BF16)
        lowp = lax.broadcasted_iota(jnp.int32, (256, 128), 1) < 64
        lhs = jnp.concatenate([jnp.where(lowp, hif, lof).astype(BF16),
                               jnp.where(lowp, hif, 0.0).astype(BF16)], 1)
        for h in range(2):
            parts = []
            for j in (2 * h, 2 * h + 1):
                pj = jnp.concatenate([hi[64 * j:64 * j + 64], lo[64 * j:64 * j + 64]], 1)
                parts += [pj, pj]
            upd = nt(lhs, jnp.concatenate(parts, 0))
            for j in range(2):
                tb[:, 2 * h + j] = tb[:, 2 * h + j] - upd[:, 128 * j:128 * j + 128].reshape(4, 64, 128)
        z = zpad[pl.ds(pl.multiple_of(64 * g, 64), 128), :]
        z_hi, z_lo = split(z)
        mix = nn(jnp.concatenate([wz_hi, wz_lo], 1), jnp.concatenate([z_hi, z_hi], 0)) + nn(wz_hi, z_lo)
        turned = pltpu.roll(m, 64, 1)
        both = jnp.where(low, turned, m)
        here = lax.broadcasted_iota(jnp.int32, (64, 256), 1) // 64 == g
        wrow = jnp.where(here, jnp.concatenate([both, both], 1), -mix)
        at = pl.ds(pl.multiple_of(64 * g, 64), 64)
        r_hi, r_lo = split(wrow)
        w_hi[at, :] = r_hi
        w_lo[at, :] = r_lo
        zpad[64:, :] = zpad[64:, :] + nn(lhs, jnp.concatenate([r_hi, r_hi, r_lo, r_lo], 0))
        return 0
    for g in range(4):
        group(g, 0)

def blocks(tile, tb):
    low = lax.broadcasted_iota(jnp.int32, (256, 128), 1) < 64
    for h in range(2):
        x = tile[:, 128 * h:128 * h + 128]
        r = pltpu.roll(x, 64, 1)
        tb[:, 2 * h] = jnp.where(low, x, r).reshape(4, 64, 128)
        tb[:, 2 * h + 1] = jnp.where(low, r, x).reshape(4, 64, 128)


B = 256
STEPS = 8
SLOTS = 10

def nt3(ah, al, bh, bl):
    return nt(ah, bh) + nt(ah, bl) + nt(al, bh)

def nn3(ah, al, bh, bl):
    return nn(ah, bh) + nn(ah, bl) + nn(al, bh)

def pair(r):
    return pl.ds(2 * r, 2)

def lead_factor(p, g, lx, lh, ll, wh, wl, tb, ud, lb, zpad, ready, ready_rest, pump):
    def apply(j, r, m):
        got = nt3(lh[m, pair(r)].reshape(512, B), ll[m, pair(r)].reshape(512, B), lh[m, j], ll[m, j])
        g[j, pair(r)] = g[j, pair(r)] - got.reshape(2, B, B)

    def step(k, _):
        ready(k)

        def last(r, _):
            def term(m, _):
                apply(k, r, m)
                return 0
            return lax.fori_loop(jnp.where(k == 2, 0, k - 1), k, term, 0)
        lax.fori_loop(jnp.where(k > 0, k // 2, 5), jnp.where(k > 0, k // 2 + 1, 5), last, 0)
        blocks(g[k, k], tb)

        def beside(i):
            below = 4 - k // 2
            now = below * jnp.where(k == 0, 0, jnp.where(k == 2, 2, 1))
            j = k + 1
            rows = jnp.maximum(5 - j // 2, 1)
            for n in range(4):
                turn = 4 * i + n
                first = turn < now
                later = jnp.maximum(turn - now, 0)
                m = later // rows
                on = (m < k) & (j < STEPS) & (j != 2)
                apply(jnp.where(first, k, jnp.where(on, j, 7)),
                      jnp.where(first, k // 2 + 1 + turn % below, jnp.where(on, j // 2 + later % rows, 0)),
                      jnp.where(first, jnp.where(k == 2, turn // below, k - 1), jnp.where(on, m, 0)))

        factor_tile(tb, ud, lb, zpad, wh, wl, lambda i: pump(k, i), beside)
        ready_rest(k)

        def solve(r):
            ah, al = split(g[k, pair(r)].reshape(512, B))
            return nt3(ah, al, wh[...], wl[...])

        def keep(r, got):
            hi, lo = split(got.reshape(2, B, B))
            lh[k, pair(r)] = hi
            ll[k, pair(r)] = lo

        got = solve(4)
        got = jnp.concatenate([jnp.where(p > k, got[:B], 0.0), got[B:]], 0)
        keep(4, got)
        lx[k] = got.reshape(2, B, B)

        @pl.when(p == k)
        def _():
            low = lax.broadcasted_iota(jnp.int32, (64, 128), 1) < 64
            tri = lax.broadcasted_iota(jnp.int32, (64, 128), 0) <= lax.broadcasted_iota(jnp.int32, (64, 128), 1)
            for i in range(4):
                up = jnp.where(tri & low, ud[i], 0.0)
                turned = jnp.concatenate([up, jnp.zeros((64, 128), F32)], 0).T[:64]
                twice = turned + pltpu.roll(turned, 64, 1)
                parts = [lb[i, j] if j < i else (twice if j == i else jnp.zeros((64, 128), F32)) for j in range(4)]
                for h in range(2):
                    lx[k, 0, 64 * i:64 * i + 64, 128 * h:128 * h + 128] = jnp.where(low, parts[2 * h], parts[2 * h + 1])

        def rest(r, _):
            keep(r, solve(r))
            return 0
        lax.fori_loop((k + 1) // 2, 4, rest, 0)
        return 0
    lax.fori_loop(0, STEPS, step, 0)

def trail(p, q, k, lx, ly, tiles):
    def rows(ref, first):
        t = ref[k].reshape(512, B)
        return split(jnp.concatenate([jnp.where(first > k, t[:B], 0.0), t[B:]], 0))
    xh, xl = rows(lx, p)
    yh, yl = rows(ly, q)
    for a in range(2):
        tiles[a] = tiles[a] - nt3(xh[B * a:B * a + B], xl[B * a:B * a + B], yh, yl)

def put_out(q, lx, tiles, out_ref):
    @pl.when(q < STEPS)
    def _():
        tiles[:, :, :B] = lx[jnp.minimum(q, STEPS - 1)]
    for a in range(2):
        for j in range(4):
            out_ref[pl.ds(4 * B * a + j, B, stride=4), :] = tiles[a, :, 128 * j:128 * j + 128]

def scratch():
    V = pltpu.VMEM
    return [V((STEPS, SLOTS, B, B), BF16), V((STEPS, SLOTS, B, B), BF16), V((B, B), BF16), V((B, B), BF16),
            V((4, 4, 64, 128), F32), V((4, 64, 128), F32), V((4, 4, 64, 128), F32), V((320, B), F32)]
MESH = pl.DeviceIdType.MESH
HOME = 1

class Comm:
    def __init__(self, p, q, own, g, lx, ly, send_sem, g_sem, x_sem, d_sem, in_sem, out_sem, z_sem, s_sem, y_sem):
        self.p, self.q, self.own, self.g, self.lx, self.ly = p, q, own, g, lx, ly
        self.px, self.py, self.pz, self.c = p % 4, p // 4, q // 2, q % 2
        self.send_sem, self.g_sem, self.x_sem, self.d_sem = send_sem, g_sem, x_sem, d_sem
        self.in_sem, self.out_sem = in_sem, out_sem
        self.z_sem, self.s_sem, self.y_sem = z_sem, s_sem, y_sem
        self.base, self.next, self.waiting = self.layout()[0], 0, False
        self.home = self.pz == HOME

    def at_z(self, d):
        return (self.p, 2 * ((self.pz + d) % 8) + self.c)

    def at_y(self, d):
        return (4 * ((self.py + d) % 4) + self.px, self.q)

    def at_x(self, d):
        return (4 * self.py + (self.px + d) % 4, self.q)

    def sibling(self):
        return (self.p, 2 * self.pz + 1 - self.c)

    def barrier(self):
        b = pltpu.get_barrier_semaphore()
        peers = [self.at_z(d) for d in (1, -1, 2, -2)] + [self.at_y(1), self.at_y(-1), self.at_x(1), self.at_x(-1), self.sibling()]
        for d in peers:
            pl.semaphore_signal(b, inc=1, device_id=d, device_id_type=MESH)
        pl.semaphore_wait(b, len(peers))

    def copy(self, cond, src, dst, send_sem, recv_sem, to):
        c = pltpu.make_async_remote_copy(src_ref=src, dst_ref=dst, send_sem=send_sem, recv_sem=recv_sem,
                                         device_id=to, device_id_type=MESH)
        pl.when(cond)(c.wait_send if self.waiting else c.start)

    def send(self, cond, src, dst, sem, to):
        self.copy(cond, src, dst, self.send_sem.at[self.next], sem, to)
        self.next += 1

    def take(self, cond, ref, sem):
        if self.waiting:
            return
        c = pltpu.make_async_remote_copy(src_ref=ref, dst_ref=ref, send_sem=self.send_sem.at[0],
                                         recv_sem=sem, device_id=self.sibling(), device_id_type=MESH)
        pl.when(cond)(c.wait_recv)

    @staticmethod
    def count(name, args):
        if name == "arrive":
            return 8 if args[1] == 0 else 0
        if name == "x_sibling":
            return 1
        if name == "y_forward":
            return 4
        return len(args[1]) * {"x_send": 9, "x_forward": 4, "finish": 3}[name]

    @classmethod
    def layout(cls):
        every = list(cls.BEGIN) + [op for n in sorted(cls.SCHEDULE) for op in cls.SCHEDULE[n]]
        base, at = {}, 0
        for name, *args in every:
            base[name, tuple(args)] = at
            at += cls.count(name, args)
        return base, at

    def do(self, name, *args):
        self.next = self.base[name, args]
        getattr(self, name)(*args)
        assert self.next <= self.base[name, args] + self.count(name, args), (name, args)

    def drain(self, name, *args):
        self.waiting = True
        self.do(name, *args)
        self.waiting = False

    def local(self, tiles):
        def half(a, j):
            return self.own[pl.ds(4 * B * a + j, B, stride=4), :]

        for a in range(2):
            for j in range(4):
                tiles[a, :, 128 * j:128 * j + 128] = half(a, j)

        @pl.when(self.q < 8)
        def _():
            k = jnp.minimum(self.q, 7)
            for a in range(2):
                for j in range(2):
                    self.g[k, 8 + a, :, 128 * j:128 * j + 128] = half(a, j)

    def gp(self, k, slot, piece):
        return self.g.at[k, slot, pl.ds(64 * piece, 64)]

    def to_home(self):
        k = jnp.minimum(self.q, 7)
        for a in range(2):
            for piece in range(4):
                ref = self.gp(k, 8 + a, piece)
                self.copy((self.q < 8) & (self.pz != HOME), ref, ref, self.in_sem.at[a, piece],
                          self.g_sem.at[k, 8 + a, piece], (self.p, 2 * HOME + self.c))

    def arrive(self, zs, a):
        k = 2 * zs + self.c
        for piece in range(4):
            ref, sem = self.gp(k, 8 + a, piece), self.g_sem.at[k, 8 + a, piece]
            if zs != HOME:
                self.take(k < 8, ref, sem)
            if a == 0:
                row = (self.p < 8) & (k <= self.p)
                pp = jnp.minimum(self.p, 7)
                for e in (1, -1):
                    self.send(row, ref, self.gp(k, pp, piece), self.g_sem.at[k, pp, piece], self.at_y(e))

    def x_sibling(self, zs, a):
        k = 2 * zs + self.c
        self.send(k < 8, self.g.at[k, 8 + a], self.g.at[k, 8 + a], self.x_sem.at[k, a], self.sibling())

    def y_forward(self, i):
        k = 2 * i + self.c
        for d, pieces in ((1, (0, 1)), (-1, (2, 3))):
            ys = (self.py - d) % 4
            r = jnp.minimum(4 * ys + self.px, 7)
            on = (ys < 2) & (k <= r)
            for piece in pieces:
                ref, sem = self.gp(k, r, piece), self.g_sem.at[k, r, piece]
                self.take(on, ref, sem)
                self.send(on, ref, ref, sem, self.at_y(d))

    def x_send(self, i, rows):
        k = 2 * i + self.c
        for ys in rows:
            r = 4 * ys + self.px
            dist = (self.py - ys) % 4
            for piece in range(4):
                rest = (dist == 2) | (dist == (1 if piece >= 2 else 3))
                ref, sem = self.gp(k, r, piece), self.g_sem.at[k, r, piece]
                self.take(rest & (k <= r), ref, sem)
                for e in (1, -1):
                    self.send(k <= r, self.gp(k, jnp.where(r == self.p, 8, r), piece), ref, sem, self.at_x(e))
            self.send((k <= r) & (dist != 0), self.g.at[k, r], self.g.at[k, r], self.d_sem.at[k, r], self.sibling())

    def x_forward(self, i, rows):
        k = 2 * i + self.c
        for d, pieces in ((1, (0, 1)), (-1, (2, 3))):
            xs = (self.px - d) % 4
            for ys in rows:
                r = 4 * ys + xs
                for piece in pieces:
                    ref, sem = self.gp(k, r, piece), self.g_sem.at[k, r, piece]
                    self.take(k <= r, ref, sem)
                    self.send(k <= r, ref, ref, sem, self.at_x(d))

    def finish(self, i, rows):
        k = 2 * i + self.c
        for dx, pieces in ((1, (2, 3)), (3, (0, 1)), (2, (0, 1, 2, 3))):
            xs = (self.px - dx) % 4
            for ys in rows:
                r = 4 * ys + xs
                for piece in pieces:
                    self.take(k <= r, self.gp(k, r, piece), self.g_sem.at[k, r, piece])
                self.send(k <= r, self.g.at[k, r], self.g.at[k, r], self.d_sem.at[k, r], self.sibling())

    def from_sibling(self, i, rows):
        k = 2 * i + 1 - self.c
        if 0 in rows:
            self.take(k < 8, self.g.at[k, 8], self.x_sem.at[k, 0])
        for r in rows:
            self.take((k <= r) & (r != self.p), self.g.at[k, r], self.d_sem.at[k, r])
        if 7 in rows:
            self.take(k < 8, self.g.at[k, 9], self.x_sem.at[k, 1])

    BEGIN = [("arrive", 0, 0), ("x_sibling", 0, 0), ("y_forward", 0), ("arrive", 1, 0), ("x_send", 0, (0,)),
             ("x_forward", 0, (0,)), ("x_send", 0, (1,)), ("y_forward", 1), ("finish", 0, (0,))]

    SCHEDULE = {
        0: [("x_sibling", 1, 0), ("arrive", 2, 0), ("arrive", 0, 1), ("x_sibling", 0, 1)],
        1: [("x_forward", 0, (1,)), ("x_send", 1, (0,)), ("y_forward", 2)],
        2: [("x_send", 1, (1,))],
        3: [("finish", 0, (1,)), ("x_sibling", 2, 0), ("arrive", 3, 0)],
        4: [("x_forward", 1, (0,)), ("x_send", 2, (0,))],
        5: [("x_forward", 1, (1,)), ("x_send", 2, (1,)), ("y_forward", 3)],
        6: [("x_sibling", 3, 0), ("arrive", 1, 1), ("x_sibling", 1, 1)],
        7: [("finish", 1, (0, 1))],
        8: [("x_forward", 2, (0, 1)), ("x_send", 3, (0, 1))],
        9: [("arrive", 2, 1), ("x_sibling", 2, 1)],
        10: [("arrive", 3, 1), ("x_sibling", 3, 1)],
        11: [("finish", 2, (0, 1))],
        13: [("x_forward", 3, (0, 1))],
        17: [("finish", 3, (0, 1))],
    }

    def begin(self):
        for op in self.BEGIN:
            self.do(*op)

    def pump(self, k, g):
        it = 4 * k + g
        for top in range(0, 20, 4):
            @pl.when(k == top // 4)
            def _():
                for n in range(top, top + 4):
                    if n in self.SCHEDULE:
                        @pl.when(it == n)
                        def _():
                            for op in self.SCHEDULE[n]:
                                self.do(*op)

        @pl.when((g == 0) & (k >= 1))
        def _():
            self.z_pass(k - 1)
            self.source_rest(k - 1)

        @pl.when((g == 1) & (k >= 2))
        def _():
            self.u_pass(k - 2)

        @pl.when((g == 3) & (k >= 3))
        def _():
            self.v_pass(k - 3)

    def fill(self, i):
        row = jnp.minimum(self.p, 7)
        for col in (2 * i, 2 * i + 1):
            @pl.when((self.p < 8) & (col <= self.p))
            def _():
                self.g[col, row] = self.g[col, 8]

    def drain_item(self, i):
        for name, args in self.base:
            if args[0] == i:
                self.drain(name, *args)

    def ready(self, k):
        @pl.when(k == 0)
        def _():
            self.from_sibling(0, range(4))
            self.fill(0)

        for i, at in ((0, 1), (1, 2), (2, 3), (3, 5)):
            @pl.when(k == at)
            def _():
                if i > 0:
                    self.from_sibling(i, range(8))
                    self.fill(i)
                self.drain_item(i)

    def ready_rest(self, k):
        @pl.when(k == 0)
        def _():
            self.from_sibling(0, range(4, 8))

    def z_pass(self, k):
        dist = (self.pz - HOME) % 8
        for n in range(4):
            ref = self.lx.at[k, self.c, pl.ds(64 * n, 64)]
            self.take(dist != 0, ref, self.z_sem.at[k, n])
            self.copy(dist < 4, ref, ref, self.out_sem.at[k, n], self.z_sem.at[k, n], self.at_z(1))
            self.copy((dist == 0) | (dist > 5), ref, ref, self.out_sem.at[k, 4 + n], self.z_sem.at[k, n], self.at_z(-1))
            self.source(k, self.c, n, 0)

    def s_send(self, k):
        ref = self.lx.at[k, self.c]
        self.copy(self.pz != HOME, ref, ref, self.out_sem.at[k, 8], self.s_sem.at[k], self.sibling())

    def s_take(self, k):
        self.take(self.pz != HOME, self.lx.at[k, 1 - self.c], self.s_sem.at[k])

    def plane(self):
        first = self.c == 0
        u = lambda d: (jnp.where(first, 4 * ((self.py + d) % 4) + self.px, 4 * self.py + (self.px + d) % 4), self.q)
        v = lambda d: (jnp.where(first, 4 * self.py + (self.px + d) % 4, 4 * ((self.py + d) % 4) + self.px), self.q)
        y, x = (self.py - self.q // 4) % 4, (self.px - self.q % 4) % 4
        return u, v, jnp.where(first, y, x), jnp.where(first, x, y)

    def part(self, ref, k, a, n):
        return ref.at[k, a, pl.ds(64 * n, 64)]

    def source(self, k, a, n, half):
        u, v, _, _ = self.plane()
        for e, to in enumerate((u(1), u(-1), v(1), v(-1))):
            self.copy(self.p == self.q, self.part(self.lx, k, a, n), self.part(self.ly, k, a, n),
                      self.out_sem.at[k, 9 + 16 * half + 4 * n + e], self.y_sem.at[k, a, n], to)

    def source_rest(self, k):
        for n in range(4):
            self.source(k, 1 - self.c, n, 1)

    def u_pass(self, k):
        u, v, du, dv = self.plane()
        line = (dv == 0) & (du != 0)
        for half in range(2):
            a = self.c if half == 0 else 1 - self.c
            for n in range(4):
                ref, sem = self.part(self.ly, k, a, n), self.y_sem.at[k, a, n]
                self.take(line, ref, sem)
                at = 9 + 12 * half + 3 * n
                self.copy(line, ref, ref, self.out_sem.at[k, at], sem, v(1))
                self.copy(line, ref, ref, self.out_sem.at[k, at + 1], sem, v(-1))
                self.copy(line & (du == (1 if n < 2 else 3)), ref, ref, self.out_sem.at[k, at + 2], sem, u(1 if n < 2 else -1))

    def v_pass(self, k):
        u, v, du, dv = self.plane()
        for half in range(2):
            a = self.c if half == 0 else 1 - self.c
            for n in range(4):
                ref, sem = self.part(self.ly, k, a, n), self.y_sem.at[k, a, n]
                self.take(dv != 0, ref, sem)
                self.copy(dv == (1 if n < 2 else 3), ref, ref, self.out_sem.at[k, 9 + 4 * half + n], sem, v(1 if n < 2 else -1))

        @pl.when((self.p == self.q) & (not self.waiting))
        def _():
            self.ly[k] = self.lx[k]

    def end(self):
        @pl.when(self.home)
        def _():
            for name, args in self.base:
                if args[0] not in (0, 1, 2, 3):
                    self.drain(name, *args)

        self.waiting = True
        self.to_home()
        self.waiting = False

        def one(k, _):
            self.drain_step(k)
            return 0
        lax.fori_loop(jnp.where(self.home, 0, 5), STEPS, one, 0)

    def drain_step(self, k):
        self.waiting = True
        self.z_pass(k)
        self.s_send(k)
        self.source_rest(k)
        self.u_pass(k)
        self.v_pass(k)
        self.waiting = False

def comm_scratch():
    D = pltpu.SemaphoreType.DMA
    return [D((Comm.layout()[1],)), D((8, 10, 4)), D((8, 2)), D((8, 8)), D((2, 4)), D((8, 41)), D((8, 4)), D((8,)), D((8, 2, 4))]

from jax.sharding import PartitionSpec as P


def entry(own, out_ref, g, lx, ly, tiles, *rest):
    p, q = lax.axis_index("row"), lax.axis_index("col")
    n = len(comm_scratch())
    comm = Comm(p, q, own, g, lx, ly, *rest[:n])
    comm.local(tiles)
    comm.barrier()
    comm.to_home()

    @pl.when(comm.home)
    def _():
        comm.begin()
        lead_factor(p, g, lx, *rest[n:], comm.ready, comm.ready_rest, comm.pump)
        comm.z_pass(7)
        comm.source_rest(7)
        comm.u_pass(6)
        comm.v_pass(5)

        def old(k, _):
            trail(p, q, k, lx, ly, tiles)
            return 0
        lax.fori_loop(0, 6, old, 0)
        comm.u_pass(7)
        comm.v_pass(6)
        trail(p, q, 6, lx, ly, tiles)

    @pl.when(jnp.logical_not(comm.home))
    def _():
        def turn(n, _):
            @pl.when(n < 8)
            def _():
                comm.z_pass(n)
                comm.s_send(n)
                comm.s_take(n)
                comm.source_rest(n)

            @pl.when((n >= 1) & (n < 9))
            def _():
                comm.u_pass(n - 1)

            @pl.when((n >= 2) & (n < 9))
            def _():
                comm.v_pass(n - 2)
                trail(p, q, n - 2, lx, ly, tiles)

            @pl.when((n >= 3) & (n < 8))
            def _():
                comm.drain_step(n - 3)
            return 0
        lax.fori_loop(0, 9, turn, 0)

    comm.v_pass(7)
    trail(p, q, 7, lx, ly, tiles)
    put_out(q, lx, tiles, out_ref)
    comm.end()


def on_device(matrix):
    out = pl.pallas_call(
        entry,
        out_shape=jax.ShapeDtypeStruct((8 * B, 128), F32),
        in_specs=[pl.BlockSpec(memory_space=pltpu.VMEM)],
        out_specs=pl.BlockSpec(memory_space=pltpu.VMEM),
        scratch_shapes=[pltpu.VMEM((STEPS, SLOTS, B, B), F32), pltpu.VMEM((STEPS, 2, B, B), F32),
                        pltpu.VMEM((STEPS, 2, B, B), F32), pltpu.VMEM((2, B, 2 * B), F32)] + comm_scratch() + scratch(),
        compiler_params=pltpu.CompilerParams(vmem_limit_bytes=63 * 1024 * 1024, collective_id=0, has_side_effects=True),
        name="steps",
    )(matrix.reshape(8 * B, 128))
    return out.reshape(matrix.shape)


def solution(mesh):
    spec = P(None, "row", None, None, "col", None)
    return jax.shard_map(on_device, mesh=mesh, in_specs=(spec,), out_specs=spec, check_vma=False)
```
